256 devices in a mesh: band: 16 (over z, y_lo), grid: 16 (over x, y_hi, core).
Axes of the slice: x: 4, y: 4 (y_hi: 2, y_lo: 2; y = y_hi * 2 + y_lo), z: 8, core: 2. Of those that a mesh axis runs over, the one named last changes fastest.
Arguments:
- orbitals: bfloat16 [16, 128, 128, 128], P('band', 'grid'), may hold values from -3 to 3
- trial_vectors: bfloat16 [2, 16, 128, 128, 128], P(None, 'band', 'grid'), may hold values from -6 to 6
- alda_kernel: float32 [128, 128, 128], P('grid'), may hold values from -2 to -0.5
- local_potential: float32 [128, 128, 128], P('grid'), may hold values from -2 to 1
- band_energies: float32 [16], P('band'), may hold values from -1.5 to -0.2
Outputs:
- sigma_real: float32 [2, 16, 128, 128, 128], P(None, 'band', 'grid')
- sigma_imag: float32 [2, 16, 128, 128, 128], P(None, 'band', 'grid')
The draws below stay inside these ranges and needn't reach their ends.
All inputs are finite; a program needn't handle non-finite values.
Results may differ from the reference program's by a relative error of at most 0.0003.
Values sent between devices are 32-bit elements; how exact they have to be, the bound alone decides.
No kernel may reach another device: no remote copies, remote signals or barrier semaphores. Data moves between devices by JAX's collectives and lax.ppermute only.
A program may use at most 64 MiB of HBM per device.

```python
import math
import jax
import jax.numpy as jnp
from jax import lax

NG = 128
TRIALS = 2
BANDS = 16


def levels(own_key, extent, split, smallest, largest):
    def one(dim, parts):
        steps = jax.random.uniform(jax.random.fold_in(jax.random.fold_in(own_key, 6), dim), (parts,), jnp.float32, smallest / len(split), largest / len(split))
        return jnp.repeat(jnp.exp(steps), extent[dim] // parts).reshape((-1,) + (1,) * (len(extent) - dim - 1))

    gain = one(*split[0])
    for cut in split[1:]:
        gain = gain * one(*cut)
    return gain


def gaussian(own_key, extent, spread, most, cuts=(), kind=jnp.bfloat16):
    drawn = spread * jax.random.normal(own_key, extent, jnp.float32)
    if cuts:
        drawn = drawn * levels(own_key, extent, cuts, -0.22, 0.18)
    return jnp.clip(drawn, -most, most).astype(kind)


def setup_inputs(seed: int = 0) -> dict:
    keys = jax.random.split(jax.random.key(seed), 6)
    return {
        "orbitals": gaussian(keys[0], (BANDS, NG, NG, NG), 0.5, 3.0, ((0, 16), (1, 16))),
        "trial_vectors": gaussian(keys[1], (TRIALS, BANDS, NG, NG, NG), 1.0, 6.0, ((1, 16), (2, 16))),
        "alda_kernel": jnp.clip(-2.0 + 1.5 * jax.random.uniform(keys[2], (NG, NG, NG), jnp.float32) ** levels(keys[2], (NG, NG, NG), ((0, 16),), -0.2, 0.2), -2.0, -0.5),
        "local_potential": jnp.clip(-2.0 + 3.0 * jax.random.uniform(keys[3], (NG, NG, NG), jnp.float32) ** levels(keys[3], (NG, NG, NG), ((0, 16),), -0.2, 0.2), -2.0, 1.0),
        "band_energies": jnp.clip(-1.5 + 1.3 * jax.random.uniform(keys[4], (BANDS,), jnp.float32) ** levels(keys[4], (BANDS,), ((0, 16),), -0.2, 0.2), -1.5, -0.2),
    }


box_length = 30.0


def frequency(length):
    positions = jnp.arange(length, dtype=jnp.int32)
    signed = jnp.where(2 * positions < length, positions, positions - length)
    return signed.astype(jnp.float32)


def coulomb(length):
    signed = frequency(length)
    squared = signed[:, None, None] ** 2 + signed[None, :, None] ** 2 + signed[None, None, :] ** 2
    scaled = (box_length ** 2 / math.pi) / jnp.maximum(squared, 1.0)
    return jnp.where(squared > 0, scaled, 0.0).astype(jnp.float32)


def reference(orbitals, trial_vectors, alda_kernel, local_potential, band_energies):
    length = NG
    kernel = coulomb(length)
    orbital_wide = orbitals.astype(jnp.float32)
    norm_factor = float(length) ** -1.5

    def one_trial(trial_fields):
        density = 2.0 * jnp.sum(trial_fields.astype(jnp.float32) * orbital_wide, axis=0)
        spectrum = jnp.fft.fftn(density) * kernel
        hartree = jnp.real(jnp.fft.ifftn(spectrum)).astype(jnp.float32)
        potential = hartree + alda_kernel * density

        def one_band(member):
            orbital, trial_field, energy = member
            fields = potential * orbital + (local_potential - energy) * trial_field.astype(jnp.float32)
            transformed = jnp.transpose(jnp.fft.fftn(fields), (1, 2, 0)) * norm_factor
            return jnp.real(transformed).astype(jnp.float32), jnp.imag(transformed).astype(jnp.float32)

        return lax.map(one_band, (orbital_wide, trial_fields, band_energies))

    real_parts, imag_parts = lax.map(one_trial, trial_vectors)
    return (real_parts, imag_parts)
```

```python
import functools
import math

import jax
import jax.numpy as jnp
import numpy as np
from jax import lax
from jax.experimental import pallas as pl
from jax.experimental.pallas import tpu as pltpu
from jax.sharding import PartitionSpec as P

box_length = 30.0
NARROW = jnp.bfloat16
WIDE = jnp.float32


def halves(table):
    high = table.astype(np.float32).astype(jnp.bfloat16)
    low = (table - high.astype(np.float64)).astype(np.float32).astype(jnp.bfloat16)
    return np.stack([high, low])


def waves(rows, columns, period):
    wrapped = np.outer(np.asarray(rows), np.asarray(columns)) % period
    angles = wrapped.astype(np.float64) * (2.0 * math.pi / period)
    return np.cos(angles), np.sin(angles)


@functools.cache
def make_tables(length, parts):
    share = length // parts
    cosine, sine = waves(range(length), range(length), length)
    norm = float(length) ** -1.5
    out = {}
    out["share_forward"] = halves(np.concatenate([cosine, -sine], 0))
    out["share_back"] = halves(np.concatenate([cosine, -sine], 0))
    out["field_z"] = halves(np.concatenate([cosine, -sine], 1))
    out["field_y"] = halves(np.block([[cosine, sine], [-sine, cosine]]))
    out["field_x"] = halves(np.block([[cosine, -sine], [sine, cosine]]) * norm)
    pieces = np.arange(parts)
    outer, inner = np.repeat(pieces, parts), np.tile(pieces, parts)
    turns = np.outer(outer, outer) + np.outer(inner, inner)
    angles = 2.0 * math.pi * (turns % parts) / parts
    out["plane_rows"] = halves(np.concatenate([np.cos(angles), -np.sin(angles)], 0))
    steps = np.arange(share)
    first, second = np.repeat(steps, share), np.tile(steps, share)
    turns = np.outer(outer, second) + np.outer(inner, first)
    angles = 2.0 * math.pi * turns / length
    out["twist"] = np.stack(
        [np.tile(np.cos(angles), (1, 2)), np.tile(-np.sin(angles), (1, 2))]
    ).astype(np.float32)
    turns = np.outer(first, first) + np.outer(second, second)
    angles = 2.0 * math.pi * (turns % share) / share
    real, imag = np.cos(angles), -np.sin(angles)
    out["plane_lanes"] = halves(np.block([[real, imag], [-imag, real]]))
    out["plane_lanes_back"] = halves(np.block([[real, -imag], [imag, real]]))
    return out


def split(value):
    high = value.astype(NARROW)
    return high, (value - high.astype(WIDE)).astype(NARROW)


def mul(left, right, dims=((1,), (0,))):
    return lax.dot_general(left, right, (dims, ((), ())), preferred_element_type=WIDE)


def product(left, right, dims=((1,), (0,))):
    left_high, left_low = left
    right_high, right_low = right
    return (
        mul(left_high, right_high, dims)
        + mul(left_low, right_high, dims)
        + mul(left_high, right_low, dims)
    )


def pair(ref):
    return ref[0], ref[1]


def density_kernel(orbital_ref, trial_ref, out_ref):
    for x in range(orbital_ref.shape[1]):
        orbital = orbital_ref[0, x].astype(WIDE)
        for k in range(trial_ref.shape[0]):
            value = 2.0 * (trial_ref[k, 0, x].astype(WIDE) * orbital)
            out_ref[:, k, x] = value.reshape(out_ref.shape[0], *out_ref.shape[3:])


def density(orbitals, trials, parts):
    bands, rows, length, _ = orbitals.shape
    count = trials.shape[0]
    share = length // parts
    step = 2
    return pl.pallas_call(
        density_kernel,
        grid=(rows // step,),
        out_shape=jax.ShapeDtypeStruct((parts, count, rows, share, length), WIDE),
        in_specs=[
            pl.BlockSpec((1, step, length, length), lambda i: (0, i, 0, 0)),
            pl.BlockSpec((count, 1, step, length, length), lambda i: (0, 0, i, 0, 0)),
        ],
        out_specs=pl.BlockSpec((parts, count, step, share, length), lambda i: (0, 0, i, 0, 0)),
        name="density",
    )(orbitals, trials)


def share_forward_kernel(pieces_ref, table_ref, share_ref, out_ref):
    total = pieces_ref[0]
    for i in range(1, pieces_ref.shape[0]):
        total = total + pieces_ref[i]
    share_ref[...] = total
    length = total.shape[1]
    points = total.shape[0] // 2
    turned = product(pair(table_ref), split(total), ((1,), (1,)))
    for k in range(2):
        columns = slice(k * points, (k + 1) * points)
        out_ref[k * length : (k + 1) * length, :] = jnp.concatenate(
            [turned[:length, columns], turned[length:, columns]], axis=1
        )


def times_i(value):
    half = value.shape[1] // 2
    return jnp.concatenate([-value[:, half:], value[:, :half]], axis=1)


def plane_kernel(pieces_ref, kernel_ref, rows_ref, twist_ref, lanes_ref, back_ref, out_ref):
    count = pieces_ref.shape[0]
    rows = pair(rows_ref)
    turned = product(rows, split(pieces_ref[...]))
    value = turned[:count] + times_i(turned[count:])
    value = value * twist_ref[0] + times_i(value) * twist_ref[1]
    value = product(split(value), pair(lanes_ref))
    value = value * kernel_ref[...]
    value = product(split(value), pair(back_ref))
    value = value * twist_ref[0] - times_i(value) * twist_ref[1]
    turned = product(rows, split(value))
    out_ref[...] = turned[:count] - times_i(turned[count:])


def share_back_kernel(pieces_ref, table_ref, share_ref, alda_ref, out_ref):
    length = table_ref.shape[2]
    points = share_ref.shape[0] // 2
    rows = []
    for k in range(2):
        turned = pieces_ref[k * length : (k + 1) * length, :].T
        rows.append(jnp.concatenate([turned[:points], turned[points:]], axis=1))
    value = product(split(jnp.concatenate(rows, axis=0)), pair(table_ref))
    alda = jnp.concatenate([alda_ref[...], alda_ref[...]], axis=0)
    value = value + alda * share_ref[...]
    for i in range(out_ref.shape[0]):
        out_ref[i] = value


def field_kernel(
    energy_ref, potential_ref, orbital_ref, trial_ref, local_ref, z_ref, y_ref, out_ref
):
    length = orbital_ref.shape[2]
    parts = potential_ref.shape[0]
    energy = energy_ref[0]
    for x in range(orbital_ref.shape[1]):
        orbital = orbital_ref[0, x].astype(WIDE)
        weight = local_ref[x] - energy
        fields = []
        for k in range(2):
            potential = potential_ref[:, k, x].reshape(length, length)
            fields.append(potential * orbital + weight * trial_ref[k, 0, x].astype(WIDE))
        turned = product(split(jnp.concatenate(fields, axis=0)), pair(z_ref))
        real = jnp.concatenate([turned[:length, :length], turned[length:, :length]], axis=1)
        imag = jnp.concatenate([turned[:length, length:], turned[length:, length:]], axis=1)
        turned = product(pair(y_ref), split(jnp.concatenate([real, imag], axis=0)))
        for k in range(2):
            for part in range(2):
                block = turned[part * length : (part + 1) * length, k * length : (k + 1) * length]
                out_ref[:, k, part, x] = block.reshape(parts, length // parts, length)


def final_kernel(pieces_ref, x_ref, real_ref, imag_ref):
    length = real_ref.shape[-1]
    share = real_ref.shape[2]
    table = pair(x_ref)
    for k in range(2):
        for b in range(share):
            parts = []
            for part in range(2):
                start = (k * 2 + part) * share * share + b
                block = pieces_ref[:, pl.ds(start, share, stride=share), :]
                parts.append(block.reshape(length, length))
            turned = product(split(jnp.concatenate(parts, axis=0).T), table)
            real_ref[k, 0, b] = turned[:, :length]
            imag_ref[k, 0, b] = turned[:, length:]


def signed(positions, length):
    return jnp.where(2 * positions < length, positions, positions - length).astype(WIDE)


def plane_coulomb(c, length, parts):
    share = length // parts
    row = lax.broadcasted_iota(jnp.int32, (parts * parts, 2 * share * share), 0)
    lane = lax.broadcasted_iota(jnp.int32, (parts * parts, 2 * share * share), 1)
    lane = lane % (share * share)
    a = row % parts + parts * (lane // share)
    b = row // parts + parts * (lane % share)
    squared = signed(a, length) ** 2 + signed(b, length) ** 2 + signed(c, length) ** 2
    scaled = box_length**2 / math.pi / jnp.maximum(squared, 1.0)
    return jnp.where(squared > 0, scaled, 0.0) / float(length**3)


def call(body, shapes, name):
    return pl.pallas_call(
        body,
        out_shape=jax.tree.map(lambda s: jax.ShapeDtypeStruct(s, WIDE), shapes, is_leaf=lambda s: isinstance(s, tuple) and isinstance(s[0], int)),
        name=name,
    )


def exchange(array, axes):
    return lax.all_to_all(array, axes, split_axis=0, concat_axis=0, tiled=True)


def per_device(orbitals, trials, alda_kernel, local_potential, band_energies):
    length = orbitals.shape[2]
    parts = lax.axis_size("band")
    share = length // parts
    points = share * share
    count = trials.shape[0]
    everyone = ("band", "grid")
    tables = {name: jnp.asarray(table) for name, table in make_tables(length, parts).items()}
    me = lax.axis_index("band")
    here = me * parts + lax.axis_index("grid")
    kernel = plane_coulomb(here % length, length, parts)
    alda = lax.dynamic_slice_in_dim(alda_kernel, me * share, share, 1).reshape(points, length)

    pieces = density(orbitals, trials, parts).reshape(parts, count * points, length)
    pieces = exchange(pieces, "band")
    density_share, planes = call(
        share_forward_kernel,
        [(count * points, length), (count * length, 2 * points)],
        "share_forward",
    )(pieces, tables["share_forward"])
    planes = exchange(planes.reshape(-1, 1, 2 * points), everyone).reshape(-1, 2 * points)
    planes = call(plane_kernel, planes.shape, "plane")(
        planes,
        kernel,
        tables["plane_rows"],
        tables["twist"],
        tables["plane_lanes"],
        tables["plane_lanes_back"],
    )
    planes = exchange(planes.reshape(-1, 1, 2 * points), everyone).reshape(-1, 2 * points)
    potential = call(share_back_kernel, (parts, count * points, length), "share_back")(
        planes, tables["share_back"], density_share, alda
    )
    potential = exchange(potential, "band").reshape(parts, count, share, share, length)

    step = 2
    fields = pl.pallas_call(
        field_kernel,
        grid=(share // step,),
        out_shape=jax.ShapeDtypeStruct((parts, count, 2, share, share, length), WIDE),
        in_specs=[
            pl.BlockSpec(memory_space=pltpu.SMEM),
            pl.BlockSpec((parts, count, step, share, length), lambda i: (0, 0, i, 0, 0)),
            pl.BlockSpec((1, step, length, length), lambda i: (0, i, 0, 0)),
            pl.BlockSpec((count, 1, step, length, length), lambda i: (0, 0, i, 0, 0)),
            pl.BlockSpec((step, length, length), lambda i: (i, 0, 0)),
            pl.BlockSpec((2, length, 2 * length), lambda i: (0, 0, 0)),
            pl.BlockSpec((2, 2 * length, 2 * length), lambda i: (0, 0, 0)),
        ],
        out_specs=pl.BlockSpec(
            (parts, count, 2, step, share, length), lambda i: (0, 0, 0, i, 0, 0)
        ),
        name="field",
    )(
        band_energies,
        potential,
        orbitals,
        trials,
        local_potential,
        tables["field_z"],
        tables["field_y"],
    )
    received = exchange(fields.reshape(parts, count * 2 * points, length), "grid")
    shape = (count, 1, share, length, length)
    return tuple(call(final_kernel, [shape, shape], "final")(received, tables["field_x"]))


def solution(mesh):
    placed = (
        P("band", "grid", None, None),
        P(None, "band", "grid", None, None),
        P("grid", None, None),
        P("grid", None, None),
        P("band"),
    )
    return jax.shard_map(
        per_device,
        mesh=mesh,
        in_specs=placed,
        out_specs=(P(None, "band", "grid", None, None), P(None, "band", "grid", None, None)),
        check_vma=False,
    )
```

```python
import functools
import math

import jax
import jax.numpy as jnp
import numpy as np
from jax import lax
from jax.experimental import pallas as pl
from jax.experimental.pallas import tpu as pltpu
from jax.sharding import PartitionSpec as P

box_length = 30.0
NARROW = jnp.bfloat16
WIDE = jnp.float32
ROWS = 2
GRANT = 20 * 2**20


def halves(table):
    high = table.astype(np.float32).astype(jnp.bfloat16)
    low = (table - high.astype(np.float64)).astype(np.float32).astype(jnp.bfloat16)
    return np.stack([high, low])


@functools.cache
def make_tables(length):
    wrapped = np.outer(np.arange(length), np.arange(length)) % length
    angles = wrapped.astype(np.float64) * (2.0 * math.pi / length)
    cosine, sine = np.cos(angles), np.sin(angles)
    return {
        "down": halves(np.block([[cosine, sine], [-sine, cosine]])),
        "up": halves(np.block([[cosine, -sine], [sine, cosine]])),
        "last": halves(np.block([[cosine, -sine], [sine, cosine]]) * float(length) ** -1.5),
    }


def split(value):
    high = value.astype(NARROW)
    return high, (value - high.astype(WIDE)).astype(NARROW)


def mul(left, right):
    return lax.dot_general(left, right, (((1,), (0,)), ((), ())), preferred_element_type=WIDE)


def product(left, right):
    left_high, left_low = left
    right_high, right_low = right
    return mul(left_high, right_high) + mul(left_low, right_high) + mul(left_high, right_low)


def pair(ref):
    return ref[0], ref[1]


def swap_blocks(value):
    rows, columns = value.shape[0] // 2, value.shape[1] // 2
    left = jnp.concatenate([value[:rows, :columns], value[rows:, :columns]], axis=1)
    right = jnp.concatenate([value[:rows, columns:], value[rows:, columns:]], axis=1)
    return jnp.concatenate([left, right], axis=0)


def parts_down(value):
    half = value.shape[1] // 2
    return jnp.concatenate([value[:, :half], value[:, half:]], axis=0)


def parts_across(value):
    half = value.shape[0] // 2
    return jnp.concatenate([value[:half], value[half:]], axis=1)


def density_kernel(orbital_ref, trial_ref, up_ref, down_ref, out_ref):
    length = orbital_ref.shape[2]
    parts, share = out_ref.shape[0], out_ref.shape[3]
    rows = orbital_ref.shape[1]
    values = []
    for x in range(rows):
        orbital = 2.0 * orbital_ref[0, x].astype(WIDE)
        values.append(
            jnp.concatenate([trial_ref[k, 0, x].astype(WIDE) * orbital for k in range(2)], axis=1)
        )
    turned = product(split(jnp.concatenate(values, axis=0)), pair(up_ref))
    columns = [parts_down(turned[x * length : (x + 1) * length]) for x in range(rows)]
    turned = product(pair(down_ref), split(jnp.concatenate(columns, axis=1)))
    for x in range(rows):
        for part in range(2):
            block = turned[part * length : (part + 1) * length, x * length : (x + 1) * length]
            out_ref[:, part, x] = block.reshape(parts, share, length)


def share_kernel(pieces_ref, share_ref, out_ref):
    total = pieces_ref[0]
    for i in range(1, pieces_ref.shape[0]):
        total = total + pieces_ref[i]
    share_ref[...] = total
    copies, rows, _ = out_ref.shape
    share = rows // 2
    for b in range(share):
        block = share_ref[pl.ds(b, rows, stride=share), :]
        for i in range(copies // share):
            out_ref[b * (copies // share) + i] = block


def line_kernel(pieces_ref, kernel_ref, down_ref, up_ref, out_ref):
    parts, rows, length = pieces_ref.shape
    share = rows // 2
    columns = jnp.concatenate(
        [pieces_ref[:, :share, :].reshape(length, length), pieces_ref[:, share:, :].reshape(length, length)],
        axis=0,
    )
    turned = product(pair(down_ref), split(columns))
    kernel = kernel_ref[...]
    turned = turned * jnp.concatenate([kernel, kernel], axis=0)
    out_ref[...] = product(pair(up_ref), split(turned)).reshape(parts, share, length)


def spread_kernel(pieces_ref, out_ref):
    share = pieces_ref.shape[0] // out_ref.shape[0]
    for part in range(2):
        for x in range(share):
            block = pieces_ref[pl.ds(part * share + x, share, stride=2 * share), :]
            rows = pl.ds((part * share + x) * share, share)
            for i in range(out_ref.shape[0]):
                out_ref[i, rows, :] = block


def back(blocks, up_ref, down_ref, length):
    turned = product(pair(up_ref), split(blocks))
    rows = turned.shape[1] // length
    points = [parts_across(turned[:, x * length : (x + 1) * length]) for x in range(rows)]
    return product(split(jnp.concatenate(points, axis=0)), pair(down_ref))


def reverse_bits(value, count):
    out = 0
    for i in range(count):
        out = out + (((value >> i) & 1) << (count - 1 - i))
    return out


def base_kernel(
    me_ref, energy_ref, near_ref, far_ref, orbital_ref, trial_ref, alda_ref, local_ref,
    up_ref, down_ref, out_ref,
):
    length = orbital_ref.shape[2]
    parts = 2 * near_ref.shape[0]
    share = length // parts
    bits = parts.bit_length() - 1
    me = me_ref[0]
    energy = energy_ref[0]
    even = (me & 1) == 0
    scale = 1.0 / float(length * length)
    rows = orbital_ref.shape[1]
    columns = []
    for x in range(rows):
        tiles = []
        for part in range(2):
            for half in range(parts // 2):
                slot = reverse_bits((half ^ (me >> 1)) << 1, bits)
                near = near_ref[slot, part, x]
                far = far_ref[slot, part, x]
                tiles.append(jnp.where(even, near, far))
                tiles.append(jnp.where(even, far, near))
        columns.append(jnp.concatenate(tiles, axis=0))
    value = back(jnp.concatenate(columns, axis=1), up_ref, down_ref, length)
    for x in range(rows):
        factor = orbital_ref[0, x].astype(WIDE) * (alda_ref[x] * scale)
        weight = local_ref[x] - energy
        for k in range(2):
            block = value[x * length : (x + 1) * length, k * length : (k + 1) * length]
            out_ref[k, x] = block * factor + weight * trial_ref[k, 0, x].astype(WIDE)


def field_kernel(potential_ref, orbital_ref, base_ref, up_ref, down_ref, out_ref):
    length = orbital_ref.shape[2]
    parts = potential_ref.shape[0]
    rows = orbital_ref.shape[1]
    columns = []
    for x in range(rows):
        columns.append(
            jnp.concatenate(
                [potential_ref[:, part, x].reshape(length, length) for part in range(2)], axis=0
            )
        )
    value = back(jnp.concatenate(columns, axis=1), up_ref, down_ref, length)
    fields = []
    for x in range(rows):
        orbital = orbital_ref[0, x].astype(WIDE)
        for k in range(2):
            block = value[x * length : (x + 1) * length, k * length : (k + 1) * length]
            fields.append(block * orbital + base_ref[k, x])
    table = (up_ref[0, :length, :], up_ref[1, :length, :])
    turned = product(split(jnp.concatenate(fields, axis=0)), table)
    for x in range(rows):
        points = swap_blocks(turned[2 * x * length : 2 * (x + 1) * length])
        waves = product(pair(down_ref), split(points))
        for k in range(2):
            for part in range(2):
                block = waves[part * length : (part + 1) * length, k * length : (k + 1) * length]
                out_ref[:, k, part, x] = block.reshape(parts, length // parts, length)


def final_kernel(pieces_ref, x_ref, real_ref, imag_ref):
    length = real_ref.shape[-1]
    share = real_ref.shape[2]
    table = pair(x_ref)
    for k in range(2):
        for b in range(share):
            parts = []
            for part in range(2):
                start = (k * 2 + part) * share * share + b
                block = pieces_ref[:, pl.ds(start, share, stride=share), :]
                parts.append(block.reshape(length, length))
            turned = product(split(jnp.concatenate(parts, axis=0).T), table)
            real_ref[k, 0, b] = turned[:, :length]
            imag_ref[k, 0, b] = turned[:, length:]


def signed(positions, length):
    return jnp.where(2 * positions < length, positions, positions - length).astype(WIDE)


def line_coulomb(b, length):
    a = lax.broadcasted_iota(jnp.int32, (length, length), 0)
    c = lax.broadcasted_iota(jnp.int32, (length, length), 1)
    squared = signed(a, length) ** 2 + signed(b, length) ** 2 + signed(c, length) ** 2
    scaled = box_length**2 / math.pi / jnp.maximum(squared, 1.0)
    return jnp.where(squared > 0, scaled, 0.0) / float(length**3)


def call(body, shapes, name, **options):
    return pl.pallas_call(
        body,
        out_shape=jax.tree.map(
            lambda s: jax.ShapeDtypeStruct(s, WIDE),
            shapes,
            is_leaf=lambda s: isinstance(s, tuple) and isinstance(s[0], int),
        ),
        name=name,
        compiler_params=pltpu.CompilerParams(vmem_limit_bytes=GRANT),
        **options,
    )


def exchange(array, axes):
    return lax.all_to_all(array, axes, split_axis=0, concat_axis=0, tiled=True)


def partner(array, axis, mask):
    return lax.ppermute(array, axis, [(i, i ^ mask) for i in range(lax.axis_size(axis))])


def per_device(orbitals, trials, alda_kernel, local_potential, band_energies):
    length = orbitals.shape[2]
    parts = lax.axis_size("band")
    share = length // parts
    points = share * share
    tables = {name: jnp.asarray(table) for name, table in make_tables(length).items()}
    me = lax.axis_index("band")
    place = lax.axis_index("grid")
    copies = parts // share
    kernel = line_coulomb(me * share + place // copies, length)
    own_up = lax.dynamic_slice_in_dim(tables["up"], (place % copies) * length, length, 1)

    scalar = pl.BlockSpec(memory_space=pltpu.SMEM)
    orbital_block = pl.BlockSpec((1, ROWS, length, length), lambda i: (0, i, 0, 0))
    trial_block = pl.BlockSpec((2, 1, ROWS, length, length), lambda i: (0, 0, i, 0, 0))
    table_block = pl.BlockSpec((2, 2 * length, 2 * length), lambda i: (0, 0, 0))
    share_block = pl.BlockSpec((parts, 2, ROWS, share, length), lambda i: (0, 0, i, 0, 0))
    half_block = pl.BlockSpec((parts // 2, 2, ROWS, share, length), lambda i: (0, 0, i, 0, 0))
    local_block = pl.BlockSpec((ROWS, length, length), lambda i: (i, 0, 0))
    base_block = pl.BlockSpec((2, ROWS, length, length), lambda i: (0, i, 0, 0))
    steps = (share // ROWS,)

    pieces = call(
        density_kernel,
        (parts, 2, share, share, length),
        "density",
        grid=steps,
        in_specs=[orbital_block, trial_block, table_block, table_block],
        out_specs=share_block,
    )(orbitals, trials, tables["up"], tables["down"])
    pieces = exchange(pieces.reshape(parts, 2 * points, length), "band")
    spectrum, lines = call(
        share_kernel, [(2 * points, length), (parts, 2 * share, length)], "share"
    )(pieces)
    masks = [parts >> (i + 1) for i in range(parts.bit_length() - 1)]
    held = spectrum[None]
    far = partner(held, "band", masks[0])
    lines, far = lax.optimization_barrier((exchange(lines, "grid"), far))
    held = jnp.concatenate([held, far], axis=0)
    far = partner(held, "band", masks[1])
    lines = call(line_kernel, (parts, share, length), "line")(
        lines, kernel, tables["down"], own_up
    )
    lines, far = lax.optimization_barrier((exchange(lines, "grid"), far))
    lines = lines.reshape(parts * share, length)
    for mask in masks[2:]:
        held = jnp.concatenate([held, far], axis=0)
        far = partner(held, "band", mask)
    potential = call(spread_kernel, (parts, 2 * points, length), "spread")(lines)
    potential = exchange(potential, "band").reshape(parts, 2, share, share, length)
    base = call(
        base_kernel,
        (2, share, length, length),
        "base",
        grid=steps,
        in_specs=[
            scalar, scalar, half_block, half_block, orbital_block, trial_block,
            local_block, local_block, table_block, table_block,
        ],
        out_specs=base_block,
    )(
        me.reshape(1),
        band_energies,
        held.reshape(parts // 2, 2, share, share, length),
        far.reshape(parts // 2, 2, share, share, length),
        orbitals,
        trials,
        alda_kernel,
        local_potential,
        tables["up"],
        tables["down"],
    )
    fields = call(
        field_kernel,
        (parts, 2, 2, share, share, length),
        "field",
        grid=steps,
        in_specs=[share_block, orbital_block, base_block, table_block, table_block],
        out_specs=pl.BlockSpec(
            (parts, 2, 2, ROWS, share, length), lambda i: (0, 0, 0, i, 0, 0)
        ),
    )(potential, orbitals, base, tables["up"], tables["down"])
    received = exchange(fields.reshape(parts, 4 * points, length), "grid")
    shape = (2, 1, share, length, length)
    return tuple(call(final_kernel, [shape, shape], "final")(received, tables["last"]))


def solution(mesh):
    placed = (
        P("band", "grid", None, None),
        P(None, "band", "grid", None, None),
        P("grid", None, None),
        P("grid", None, None),
        P("band"),
    )
    return jax.shard_map(
        per_device,
        mesh=mesh,
        in_specs=placed,
        out_specs=(P(None, "band", "grid", None, None), P(None, "band", "grid", None, None)),
        check_vma=False,
    )
```

```python
import functools
import math

import jax
import jax.numpy as jnp
import numpy as np
from jax import lax
from jax.experimental import pallas as pl
from jax.experimental.pallas import tpu as pltpu
from jax.sharding import PartitionSpec as P


box_length = 30.0
NARROW = jnp.bfloat16
WIDE = jnp.float32
ROWS = 2
GRANT = 20 * 2**20
WIDE_GRANT = 60 * 2**20


def halves(table):
    high = table.astype(np.float32).astype(jnp.bfloat16)
    low = (table - high.astype(np.float64)).astype(np.float32).astype(jnp.bfloat16)
    return np.stack([high, low])


@functools.cache
def make_tables(length):
    wrapped = np.outer(np.arange(length), np.arange(length)) % length
    angles = wrapped.astype(np.float64) * (2.0 * math.pi / length)
    cosine, sine = np.cos(angles), np.sin(angles)
    return {
        "down": halves(np.block([[cosine, sine], [-sine, cosine]])),
        "up": halves(np.block([[cosine, -sine], [sine, cosine]])),
        "last": halves(np.block([[cosine, -sine], [sine, cosine]]) * float(length) ** -1.5),
    }


def split(value):
    high = value.astype(NARROW)
    return high, (value - high.astype(WIDE)).astype(NARROW)


def mul(left, right):
    return lax.dot_general(left, right, (((1,), (0,)), ((), ())), preferred_element_type=WIDE)


def product(left, right):
    left_high, left_low = left
    right_high, right_low = right
    return mul(left_high, right_high) + mul(left_low, right_high) + mul(left_high, right_low)


def pair(ref):
    return ref[0], ref[1]


def swap_blocks(value):
    rows, columns = value.shape[0] // 2, value.shape[1] // 2
    left = jnp.concatenate([value[:rows, :columns], value[rows:, :columns]], axis=1)
    right = jnp.concatenate([value[:rows, columns:], value[rows:, columns:]], axis=1)
    return jnp.concatenate([left, right], axis=0)


def parts_down(value):
    half = value.shape[1] // 2
    return jnp.concatenate([value[:, :half], value[:, half:]], axis=0)


def parts_across(value):
    half = value.shape[0] // 2
    return jnp.concatenate([value[:half], value[half:]], axis=1)


def density_kernel(orbital_ref, trial_ref, up_ref, down_ref, out_ref):
    length = orbital_ref.shape[2]
    parts, share = out_ref.shape[0], out_ref.shape[3]
    rows = orbital_ref.shape[1]
    values = []
    for x in range(rows):
        orbital = 2.0 * orbital_ref[0, x].astype(WIDE)
        values.append(
            jnp.concatenate([trial_ref[k, 0, x].astype(WIDE) * orbital for k in range(2)], axis=1)
        )
    turned = product(split(jnp.concatenate(values, axis=0)), pair(up_ref))
    columns = [parts_down(turned[x * length : (x + 1) * length]) for x in range(rows)]
    turned = product(pair(down_ref), split(jnp.concatenate(columns, axis=1)))
    for x in range(rows):
        for part in range(2):
            block = turned[part * length : (part + 1) * length, x * length : (x + 1) * length]
            out_ref[:, part, x] = block.reshape(parts, share, length)


def share_kernel(pieces_ref, share_ref, out_ref):
    total = pieces_ref[0]
    for i in range(1, pieces_ref.shape[0]):
        total = total + pieces_ref[i]
    share_ref[...] = total
    copies, rows, _ = out_ref.shape
    share = rows // 2
    for b in range(share):
        block = share_ref[pl.ds(b, rows, stride=share), :]
        for i in range(copies // share):
            out_ref[b * (copies // share) + i] = block


def line_kernel(pieces_ref, kernel_ref, down_ref, up_ref, out_ref):
    parts, rows, length = pieces_ref.shape
    share = rows // 2
    columns = jnp.concatenate(
        [pieces_ref[:, :share, :].reshape(length, length), pieces_ref[:, share:, :].reshape(length, length)],
        axis=0,
    )
    turned = product(pair(down_ref), split(columns))
    kernel = kernel_ref[...]
    turned = turned * jnp.concatenate([kernel, kernel], axis=0)
    out_ref[...] = product(pair(up_ref), split(turned)).reshape(parts, share, length)


def spread_kernel(pieces_ref, out_ref):
    share = pieces_ref.shape[0] // out_ref.shape[0]
    for part in range(2):
        for x in range(share):
            block = pieces_ref[pl.ds(part * share + x, share, stride=2 * share), :]
            rows = pl.ds((part * share + x) * share, share)
            for i in range(out_ref.shape[0]):
                out_ref[i, rows, :] = block


def back(blocks, up_ref, down_ref, length):
    turned = product(pair(up_ref), split(blocks))
    rows = turned.shape[1] // length
    points = [parts_across(turned[:, x * length : (x + 1) * length]) for x in range(rows)]
    return product(split(jnp.concatenate(points, axis=0)), pair(down_ref))


def base_kernel(
    me_ref, energy_ref, near_ref, far_ref, orbital_ref, trial_ref, alda_ref, local_ref,
    up_ref, down_ref, out_ref,
):
    length = orbital_ref.shape[2]
    parts = 2 * near_ref.shape[0]
    me = me_ref[0]
    energy = energy_ref[0]
    even = (me & 1) == 0
    scale = 1.0 / float(length * length)
    rows = orbital_ref.shape[1]
    columns = []
    for x in range(rows):
        tiles = []
        for part in range(2):
            for half in range(parts // 2):
                slot = half ^ (me >> 1)
                near = near_ref[slot, part, x]
                far = far_ref[slot, part, x]
                tiles.append(jnp.where(even, near, far))
                tiles.append(jnp.where(even, far, near))
        columns.append(jnp.concatenate(tiles, axis=0))
    value = back(jnp.concatenate(columns, axis=1), up_ref, down_ref, length)
    for x in range(rows):
        factor = orbital_ref[0, x].astype(WIDE) * (alda_ref[x] * scale)
        weight = local_ref[x] - energy
        for k in range(2):
            block = value[x * length : (x + 1) * length, k * length : (k + 1) * length]
            out_ref[k, x] = block * factor + weight * trial_ref[k, 0, x].astype(WIDE)


def field_kernel(potential_ref, orbital_ref, base_ref, up_ref, down_ref, out_ref):
    length = orbital_ref.shape[2]
    parts = potential_ref.shape[0]
    rows = orbital_ref.shape[1]
    columns = []
    for x in range(rows):
        columns.append(
            jnp.concatenate(
                [potential_ref[:, part, x].reshape(length, length) for part in range(2)], axis=0
            )
        )
    value = back(jnp.concatenate(columns, axis=1), up_ref, down_ref, length)
    fields = []
    for x in range(rows):
        orbital = orbital_ref[0, x].astype(WIDE)
        for k in range(2):
            block = value[x * length : (x + 1) * length, k * length : (k + 1) * length]
            fields.append(block * orbital + base_ref[k, x])
    table = (up_ref[0, :length, :], up_ref[1, :length, :])
    turned = product(split(jnp.concatenate(fields, axis=0)), table)
    for x in range(rows):
        points = swap_blocks(turned[2 * x * length : 2 * (x + 1) * length])
        waves = product(pair(down_ref), split(points))
        for k in range(2):
            for part in range(2):
                block = waves[part * length : (part + 1) * length, k * length : (k + 1) * length]
                out_ref[:, k, part, x] = block.reshape(parts, length // parts, length)


def final_kernel(pieces_ref, x_ref, real_ref, imag_ref):
    length = real_ref.shape[-1]
    share = real_ref.shape[2]
    table = pair(x_ref)
    for k in range(2):
        for b in range(share):
            parts = []
            for part in range(2):
                start = (k * 2 + part) * share * share + b
                block = pieces_ref[:, pl.ds(start, share, stride=share), :]
                parts.append(block.reshape(length, length))
            turned = product(split(jnp.concatenate(parts, axis=0).T), table)
            real_ref[k, 0, b] = turned[:, :length]
            imag_ref[k, 0, b] = turned[:, length:]


def signed(positions, length):
    return jnp.where(2 * positions < length, positions, positions - length).astype(WIDE)


def line_coulomb(b, length):
    a = lax.broadcasted_iota(jnp.int32, (length, length), 0)
    c = lax.broadcasted_iota(jnp.int32, (length, length), 1)
    squared = signed(a, length) ** 2 + signed(b, length) ** 2 + signed(c, length) ** 2
    scaled = box_length**2 / math.pi / jnp.maximum(squared, 1.0)
    return jnp.where(squared > 0, scaled, 0.0) / float(length**3)


def call(body, shapes, grant=GRANT, **options):
    return pl.pallas_call(
        body,
        out_shape=jax.tree.map(
            lambda s: jax.ShapeDtypeStruct(s, WIDE),
            shapes,
            is_leaf=lambda s: isinstance(s, tuple) and isinstance(s[0], int),
        ),
        compiler_params=pltpu.CompilerParams(vmem_limit_bytes=grant),
        **options,
    )


def exchange(array, axis):
    return lax.all_to_all(array, axis, split_axis=0, concat_axis=0, tiled=True)


def partner(array, mask):
    return lax.ppermute(array, "band", [(i, i ^ mask) for i in range(lax.axis_size("band"))])


def per_device(orbitals, trials, alda_kernel, local_potential, band_energies):
    length = orbitals.shape[2]
    parts = lax.axis_size("band")
    share = length // parts
    points = share * share
    tables = {name: jnp.asarray(table) for name, table in make_tables(length).items()}
    me = lax.axis_index("band")
    place = lax.axis_index("grid")
    copies = parts // share
    kernel = line_coulomb(me * share + place // copies, length)
    own_up = lax.dynamic_slice_in_dim(tables["up"], (place % copies) * length, length, 1)

    scalar = pl.BlockSpec(memory_space=pltpu.SMEM)
    orbital_block = pl.BlockSpec((1, ROWS, length, length), lambda i: (0, i, 0, 0))
    trial_block = pl.BlockSpec((2, 1, ROWS, length, length), lambda i: (0, 0, i, 0, 0))
    table_block = pl.BlockSpec((2, 2 * length, 2 * length), lambda i: (0, 0, 0))
    share_block = pl.BlockSpec((parts, 2, ROWS, share, length), lambda i: (0, 0, i, 0, 0))
    half_block = pl.BlockSpec((parts // 2, 2, ROWS, share, length), lambda i: (0, 0, i, 0, 0))
    local_block = pl.BlockSpec((ROWS, length, length), lambda i: (i, 0, 0))
    base_block = pl.BlockSpec((2, ROWS, length, length), lambda i: (0, i, 0, 0))
    steps = (share // ROWS,)

    pieces = call(
        density_kernel,
        (parts, 2, share, share, length),
        grant=WIDE_GRANT,
        grid=steps,
        in_specs=[orbital_block, trial_block, table_block, table_block],
        out_specs=share_block,
    )(orbitals, trials, tables["up"], tables["down"])
    pieces = exchange(pieces.reshape(parts, 2 * points, length), "band")
    spectrum, lines = call(share_kernel, [(2 * points, length), (parts, 2 * share, length)])(pieces)
    lines = exchange(lines, "grid")
    held = {0: spectrum}
    for mask in (2, 4, 8):
        held[mask] = partner(spectrum, mask)
    lines, held[2], held[4], held[8] = lax.optimization_barrier((lines, held[2], held[4], held[8]))
    lines = call(line_kernel, (parts, share, length))(
        lines, kernel, tables["down"], own_up
    )
    lines = exchange(lines, "grid")
    both = partner(jnp.stack([held[4], held[8]]), 2)
    held[6], held[10] = both[0], both[1]
    held[12] = partner(held[8], 4)
    held[14] = partner(spectrum, 14)
    near = jnp.stack([held[mask] for mask in range(0, parts, 2)])
    lines, near = lax.optimization_barrier((lines, near))
    far = partner(near, 1)
    lines = lines.reshape(parts * share, length)
    potential = call(spread_kernel, (parts, 2 * points, length))(lines)
    potential = exchange(potential, "band").reshape(parts, 2, share, share, length)
    base = call(
        base_kernel,
        (2, share, length, length),
        grid=steps,
        in_specs=[
            scalar, scalar, half_block, half_block, orbital_block, trial_block,
            local_block, local_block, table_block, table_block,
        ],
        out_specs=base_block,
    )(
        me.reshape(1),
        band_energies,
        near.reshape(parts // 2, 2, share, share, length),
        far.reshape(parts // 2, 2, share, share, length),
        orbitals,
        trials,
        alda_kernel,
        local_potential,
        tables["up"],
        tables["down"],
    )
    fields = call(
        field_kernel,
        (parts, 2, 2, share, share, length),
        grid=steps,
        in_specs=[share_block, orbital_block, base_block, table_block, table_block],
        out_specs=pl.BlockSpec(
            (parts, 2, 2, ROWS, share, length), lambda i: (0, 0, 0, i, 0, 0)
        ),
    )(potential, orbitals, base, tables["up"], tables["down"])
    received = exchange(fields.reshape(parts, 4 * points, length), "grid")
    shape = (2, 1, share, length, length)
    return tuple(call(final_kernel, [shape, shape])(received, tables["last"]))


def solution(mesh):
    placed = (
        P("band", "grid", None, None),
        P(None, "band", "grid", None, None),
        P("grid", None, None),
        P("grid", None, None),
        P("band"),
    )

    return jax.shard_map(
        per_device,
        mesh=mesh,
        in_specs=placed,
        out_specs=(P(None, "band", "grid", None, None), P(None, "band", "grid", None, None)),
        check_vma=False,
    )
```

```python
import functools
import math

import jax
import jax.numpy as jnp
import numpy as np
from jax import lax
from jax.experimental import pallas as pl
from jax.experimental.pallas import tpu as pltpu
from jax.sharding import PartitionSpec as P


box_length = 30.0
NARROW = jnp.bfloat16
WIDE = jnp.float32
ROWS = 2
GRANT = 20 * 2**20
WIDE_GRANT = 60 * 2**20


def halves(table):
    high = table.astype(np.float32).astype(jnp.bfloat16)
    low = (table - high.astype(np.float64)).astype(np.float32).astype(jnp.bfloat16)
    return np.stack([high, low])


@functools.cache
def make_tables(length):
    wrapped = np.outer(np.arange(length), np.arange(length)) % length
    angles = wrapped.astype(np.float64) * (2.0 * math.pi / length)
    cosine, sine = np.cos(angles), np.sin(angles)
    return {
        "down": halves(np.block([[cosine, sine], [-sine, cosine]])),
        "up": halves(np.block([[cosine, -sine], [sine, cosine]])),
        "last": halves(np.block([[cosine, -sine], [sine, cosine]]) * float(length) ** -1.5),
    }


def split(value):
    high = value.astype(NARROW)
    return high, (value - high.astype(WIDE)).astype(NARROW)


def mul(left, right):
    return lax.dot_general(left, right, (((1,), (0,)), ((), ())), preferred_element_type=WIDE)


def product(left, right):
    left_high, left_low = left
    right_high, right_low = right
    return mul(left_high, right_high) + mul(left_low, right_high) + mul(left_high, right_low)


def pair(ref):
    return ref[0], ref[1]


def swap_blocks(value):
    rows, columns = value.shape[0] // 2, value.shape[1] // 2
    left = jnp.concatenate([value[:rows, :columns], value[rows:, :columns]], axis=1)
    right = jnp.concatenate([value[:rows, columns:], value[rows:, columns:]], axis=1)
    return jnp.concatenate([left, right], axis=0)


def parts_down(value):
    half = value.shape[1] // 2
    return jnp.concatenate([value[:, :half], value[:, half:]], axis=0)


def parts_across(value):
    half = value.shape[0] // 2
    return jnp.concatenate([value[:half], value[half:]], axis=1)


def density_kernel(orbital_ref, trial_ref, up_ref, down_ref, out_ref):
    length = orbital_ref.shape[2]
    parts, share = out_ref.shape[0], out_ref.shape[3]
    rows = orbital_ref.shape[1]
    values = []
    for x in range(rows):
        orbital = 2.0 * orbital_ref[0, x].astype(WIDE)
        values.append(
            jnp.concatenate([trial_ref[k, 0, x].astype(WIDE) * orbital for k in range(2)], axis=1)
        )
    turned = product(split(jnp.concatenate(values, axis=0)), pair(up_ref))
    columns = [parts_down(turned[x * length : (x + 1) * length]) for x in range(rows)]
    turned = product(pair(down_ref), split(jnp.concatenate(columns, axis=1)))
    for x in range(rows):
        for part in range(2):
            block = turned[part * length : (part + 1) * length, x * length : (x + 1) * length]
            out_ref[:, part, x] = block.reshape(parts, share, length)


def share_kernel(pieces_ref, share_ref, out_ref):
    total = pieces_ref[0]
    for i in range(1, pieces_ref.shape[0]):
        total = total + pieces_ref[i]
    share_ref[...] = total
    copies, rows, _ = out_ref.shape
    share = rows // 2
    for b in range(share):
        block = share_ref[pl.ds(b, rows, stride=share), :]
        for i in range(copies // share):
            out_ref[b * (copies // share) + i] = block


def line_kernel(pieces_ref, kernel_ref, down_ref, up_ref, out_ref):
    parts, rows, length = pieces_ref.shape
    share = rows // 2
    columns = jnp.concatenate(
        [pieces_ref[:, :share, :].reshape(length, length), pieces_ref[:, share:, :].reshape(length, length)],
        axis=0,
    )
    turned = product(pair(down_ref), split(columns))
    kernel = kernel_ref[...]
    turned = turned * jnp.concatenate([kernel, kernel], axis=0)
    out_ref[...] = product(pair(up_ref), split(turned)).reshape(parts, share, length)


def spread_kernel(pieces_ref, out_ref):
    share = pieces_ref.shape[0] // out_ref.shape[0]
    for part in range(2):
        for x in range(share):
            block = pieces_ref[pl.ds(part * share + x, share, stride=2 * share), :]
            rows = pl.ds((part * share + x) * share, share)
            for i in range(out_ref.shape[0]):
                out_ref[i, rows, :] = block


def back(blocks, up_ref, down_ref, length):
    turned = product(pair(up_ref), split(blocks))
    rows = turned.shape[1] // length
    points = [parts_across(turned[:, x * length : (x + 1) * length]) for x in range(rows)]
    return product(split(jnp.concatenate(points, axis=0)), pair(down_ref))


def base_kernel(
    me_ref, energy_ref, near_ref, far_ref, orbital_ref, trial_ref, alda_ref, local_ref,
    up_ref, down_ref, out_ref,
):
    length = orbital_ref.shape[2]
    parts = 2 * near_ref.shape[0]
    me = me_ref[0]
    energy = energy_ref[0]
    even = (me & 1) == 0
    scale = 1.0 / float(length * length)
    rows = orbital_ref.shape[1]
    columns = []
    for x in range(rows):
        tiles = []
        for part in range(2):
            for half in range(parts // 2):
                slot = half ^ (me >> 1)
                near = near_ref[slot, part, x]
                far = far_ref[slot, part, x]
                tiles.append(jnp.where(even, near, far))
                tiles.append(jnp.where(even, far, near))
        columns.append(jnp.concatenate(tiles, axis=0))
    value = back(jnp.concatenate(columns, axis=1), up_ref, down_ref, length)
    for x in range(rows):
        factor = orbital_ref[0, x].astype(WIDE) * (alda_ref[x] * scale)
        weight = local_ref[x] - energy
        for k in range(2):
            block = value[x * length : (x + 1) * length, k * length : (k + 1) * length]
            out_ref[k, x] = block * factor + weight * trial_ref[k, 0, x].astype(WIDE)


def field_kernel(potential_ref, orbital_ref, base_ref, up_ref, down_ref, out_ref):
    length = orbital_ref.shape[2]
    parts = potential_ref.shape[0]
    rows = orbital_ref.shape[1]
    columns = []
    for x in range(rows):
        columns.append(
            jnp.concatenate(
                [potential_ref[:, part, x].reshape(length, length) for part in range(2)], axis=0
            )
        )
    value = back(jnp.concatenate(columns, axis=1), up_ref, down_ref, length)
    fields = []
    for x in range(rows):
        orbital = orbital_ref[0, x].astype(WIDE)
        for k in range(2):
            block = value[x * length : (x + 1) * length, k * length : (k + 1) * length]
            fields.append(block * orbital + base_ref[k, x])
    table = (up_ref[0, :length, :], up_ref[1, :length, :])
    turned = product(split(jnp.concatenate(fields, axis=0)), table)
    for x in range(rows):
        points = swap_blocks(turned[2 * x * length : 2 * (x + 1) * length])
        waves = product(pair(down_ref), split(points))
        for k in range(2):
            for part in range(2):
                block = waves[part * length : (part + 1) * length, k * length : (k + 1) * length]
                out_ref[:, k, part, x] = block.reshape(parts, length // parts, length)


def final_kernel(pieces_ref, x_ref, real_ref, imag_ref):
    length = real_ref.shape[-1]
    share = real_ref.shape[2]
    table = pair(x_ref)
    for k in range(2):
        for b in range(share):
            parts = []
            for part in range(2):
                start = (k * 2 + part) * share * share + b
                block = pieces_ref[:, pl.ds(start, share, stride=share), :]
                parts.append(block.reshape(length, length))
            turned = product(split(jnp.concatenate(parts, axis=0).T), table)
            real_ref[k, 0, b] = turned[:, :length]
            imag_ref[k, 0, b] = turned[:, length:]


def signed(positions, length):
    return jnp.where(2 * positions < length, positions, positions - length).astype(WIDE)


def line_coulomb(b, length):
    a = lax.broadcasted_iota(jnp.int32, (length, length), 0)
    c = lax.broadcasted_iota(jnp.int32, (length, length), 1)
    squared = signed(a, length) ** 2 + signed(b, length) ** 2 + signed(c, length) ** 2
    scaled = box_length**2 / math.pi / jnp.maximum(squared, 1.0)
    return jnp.where(squared > 0, scaled, 0.0) / float(length**3)


def call(body, shapes, grant=GRANT, **options):
    return pl.pallas_call(
        body,
        out_shape=jax.tree.map(
            lambda s: jax.ShapeDtypeStruct(s, WIDE),
            shapes,
            is_leaf=lambda s: isinstance(s, tuple) and isinstance(s[0], int),
        ),
        compiler_params=pltpu.CompilerParams(vmem_limit_bytes=grant),
        **options,
    )


def exchange(array, axis):
    return lax.all_to_all(array, axis, split_axis=0, concat_axis=0, tiled=True)


def partner(array, mask):
    return lax.ppermute(array, "band", [(i, i ^ mask) for i in range(lax.axis_size("band"))])


def per_device(orbitals, trials, alda_kernel, local_potential, band_energies):
    length = orbitals.shape[2]
    parts = lax.axis_size("band")
    share = length // parts
    points = share * share
    tables = {name: jnp.asarray(table) for name, table in make_tables(length).items()}
    me = lax.axis_index("band")
    place = lax.axis_index("grid")
    copies = parts // share
    kernel = line_coulomb(me * share + place // copies, length)
    own_up = lax.dynamic_slice_in_dim(tables["up"], (place % copies) * length, length, 1)

    scalar = pl.BlockSpec(memory_space=pltpu.SMEM)
    orbital_block = pl.BlockSpec((1, ROWS, length, length), lambda i: (0, i, 0, 0))
    trial_block = pl.BlockSpec((2, 1, ROWS, length, length), lambda i: (0, 0, i, 0, 0))
    table_block = pl.BlockSpec((2, 2 * length, 2 * length), lambda i: (0, 0, 0))
    share_block = pl.BlockSpec((parts, 2, ROWS, share, length), lambda i: (0, 0, i, 0, 0))
    half_block = pl.BlockSpec((parts // 2, 2, ROWS, share, length), lambda i: (0, 0, i, 0, 0))
    local_block = pl.BlockSpec((ROWS, length, length), lambda i: (i, 0, 0))
    base_block = pl.BlockSpec((2, ROWS, length, length), lambda i: (0, i, 0, 0))
    steps = (share // ROWS,)

    pieces = call(
        density_kernel,
        (parts, 2, share, share, length),
        grant=WIDE_GRANT,
        grid=steps,
        in_specs=[orbital_block, trial_block, table_block, table_block],
        out_specs=share_block,
    )(orbitals, trials, tables["up"], tables["down"])
    pieces = exchange(pieces.reshape(parts, 2 * points, length), "band")
    spectrum, lines = call(share_kernel, [(2 * points, length), (parts, 2 * share, length)])(pieces)
    lines = exchange(lines, "grid")
    held = {0: spectrum}
    for mask in (2, 4, 8):
        held[mask] = partner(spectrum, mask)
    lines = call(line_kernel, (parts, share, length))(
        lines, kernel, tables["down"], own_up
    )
    lines, held[2], held[4], held[8] = lax.optimization_barrier((lines, held[2], held[4], held[8]))
    lines = exchange(lines, "grid").reshape(parts * share, length)
    both = partner(jnp.stack([held[4], held[8]]), 2)
    held[6], held[10] = both[0], both[1]
    held[12] = partner(held[8], 4)
    held[14] = partner(spectrum, 14)
    away = {}
    for masks in ((0, 2, 4, 8), (6, 10, 12, 14)):
        group = partner(jnp.stack([held[mask] for mask in masks]), 1)
        for i, mask in enumerate(masks):
            away[mask] = group[i]
    near = jnp.stack([held[mask] for mask in range(0, parts, 2)])
    far = jnp.stack([away[mask] for mask in range(0, parts, 2)])
    potential = call(spread_kernel, (parts, 2 * points, length))(lines)
    potential = exchange(potential, "band").reshape(parts, 2, share, share, length)
    base = call(
        base_kernel,
        (2, share, length, length),
        grid=steps,
        in_specs=[
            scalar, scalar, half_block, half_block, orbital_block, trial_block,
            local_block, local_block, table_block, table_block,
        ],
        out_specs=base_block,
    )(
        me.reshape(1),
        band_energies,
        near.reshape(parts // 2, 2, share, share, length),
        far.reshape(parts // 2, 2, share, share, length),
        orbitals,
        trials,
        alda_kernel,
        local_potential,
        tables["up"],
        tables["down"],
    )
    fields = call(
        field_kernel,
        (parts, 2, 2, share, share, length),
        grid=steps,
        in_specs=[share_block, orbital_block, base_block, table_block, table_block],
        out_specs=pl.BlockSpec(
            (parts, 2, 2, ROWS, share, length), lambda i: (0, 0, 0, i, 0, 0)
        ),
    )(potential, orbitals, base, tables["up"], tables["down"])
    received = exchange(fields.reshape(parts, 4 * points, length), "grid")
    shape = (2, 1, share, length, length)
    return tuple(call(final_kernel, [shape, shape])(received, tables["last"]))


def solution(mesh):
    placed = (
        P("band", "grid", None, None),
        P(None, "band", "grid", None, None),
        P("grid", None, None),
        P("grid", None, None),
        P("band"),
    )

    return jax.shard_map(
        per_device,
        mesh=mesh,
        in_specs=placed,
        out_specs=(P(None, "band", "grid", None, None), P(None, "band", "grid", None, None)),
        check_vma=False,
    )
```

```python
import functools
import math

import jax
import jax.numpy as jnp
import numpy as np
from jax import lax
from jax.experimental import pallas as pl
from jax.experimental.pallas import tpu as pltpu
from jax.sharding import PartitionSpec as P


box_length = 30.0
NARROW = jnp.bfloat16
WIDE = jnp.float32
ROWS = 8
GRANT = 20 * 2**20
WIDE_GRANT = 60 * 2**20


def halves(table):
    high = table.astype(np.float32).astype(jnp.bfloat16)
    low = (table - high.astype(np.float64)).astype(np.float32).astype(jnp.bfloat16)
    return np.stack([high, low])


@functools.cache
def make_tables(length):
    wrapped = np.outer(np.arange(length), np.arange(length)) % length
    angles = wrapped.astype(np.float64) * (2.0 * math.pi / length)
    cosine, sine = np.cos(angles), np.sin(angles)
    return {
        "down": halves(np.block([[cosine, sine], [-sine, cosine]])),
        "up": halves(np.block([[cosine, -sine], [sine, cosine]])),
        "last": halves(np.block([[cosine, -sine], [sine, cosine]]) * float(length) ** -1.5),
    }


def split(value):
    high = value.astype(NARROW)
    return high, (value - high.astype(WIDE)).astype(NARROW)


def mul(left, right):
    return lax.dot_general(left, right, (((1,), (0,)), ((), ())), preferred_element_type=WIDE)


def product(left, right):
    left_high, left_low = left
    right_high, right_low = right
    return mul(left_high, right_high) + mul(left_low, right_high) + mul(left_high, right_low)


def pair(ref):
    return ref[0], ref[1]


def swap_blocks(value):
    rows, columns = value.shape[0] // 2, value.shape[1] // 2
    left = jnp.concatenate([value[:rows, :columns], value[rows:, :columns]], axis=1)
    right = jnp.concatenate([value[:rows, columns:], value[rows:, columns:]], axis=1)
    return jnp.concatenate([left, right], axis=0)


def parts_down(value):
    half = value.shape[1] // 2
    return jnp.concatenate([value[:, :half], value[:, half:]], axis=0)


def parts_across(value):
    half = value.shape[0] // 2
    return jnp.concatenate([value[:half], value[half:]], axis=1)


def density_kernel(orbital_in, trial_in, up_in, down_in, out_hbm, *scratch):
    orbital_ref, trial_ref, up_ref, down_ref, out_ref, table_sems, row_sems, out_sems = scratch
    length = orbital_ref.shape[2]
    parts, share = out_ref.shape[0], out_ref.shape[3]
    half = orbital_ref.shape[1] // 2
    tables = [
        pltpu.make_async_copy(up_in, up_ref, table_sems.at[0]),
        pltpu.make_async_copy(down_in, down_ref, table_sems.at[1]),
    ]
    rows = [pl.ds(i * half, half) for i in range(2)]
    orbitals, trials, outs = [], [], []
    for i in range(2):
        part = (slice(None), rows[i])
        orbitals.append(
            pltpu.make_async_copy(orbital_in.at[part], orbital_ref.at[part], row_sems.at[i, 0])
        )
        part = (slice(None), slice(None), rows[i])
        trials.append(
            pltpu.make_async_copy(trial_in.at[part], trial_ref.at[part], row_sems.at[i, 1])
        )
        outs.append(pltpu.make_async_copy(out_ref.at[part], out_hbm.at[part], out_sems.at[i]))
    for copy in (tables[0], orbitals[0], trials[0], tables[1], orbitals[1], trials[1]):
        copy.start()
    for copy in tables:
        copy.wait()
    for i in range(2):
        orbitals[i].wait()
        trials[i].wait()
        values = []
        for x in range(half):
            orbital = 2.0 * orbital_ref[0, i * half + x].astype(WIDE)
            values.append(
                jnp.concatenate(
                    [trial_ref[k, 0, i * half + x].astype(WIDE) * orbital for k in range(2)], axis=1
                )
            )
        turned = product(split(jnp.concatenate(values, axis=0)), pair(up_ref))
        columns = [parts_down(turned[x * length : (x + 1) * length]) for x in range(half)]
        turned = product(pair(down_ref), split(jnp.concatenate(columns, axis=1)))
        for x in range(half):
            for part in range(2):
                block = turned[part * length : (part + 1) * length, x * length : (x + 1) * length]
                out_ref[:, part, i * half + x] = block.reshape(parts, share, length)
        outs[i].start()
    for copy in outs:
        copy.wait()


def share_kernel(pieces_ref, share_ref, out_ref):
    total = pieces_ref[0]
    for i in range(1, pieces_ref.shape[0]):
        total = total + pieces_ref[i]
    share_ref[...] = total
    copies, rows, _ = out_ref.shape
    share = rows // 2
    for b in range(share):
        block = share_ref[pl.ds(b, rows, stride=share), :]
        for i in range(copies // share):
            out_ref[b * (copies // share) + i] = block


def line_kernel(pieces_ref, kernel_ref, down_ref, up_ref, out_ref):
    parts, rows, length = pieces_ref.shape
    share = rows // 2
    columns = jnp.concatenate(
        [pieces_ref[:, :share, :].reshape(length, length), pieces_ref[:, share:, :].reshape(length, length)],
        axis=0,
    )
    turned = product(pair(down_ref), split(columns))
    kernel = kernel_ref[...]
    turned = turned * jnp.concatenate([kernel, kernel], axis=0)
    out_ref[...] = product(pair(up_ref), split(turned)).reshape(parts, share, length)


def spread_kernel(pieces_ref, out_ref):
    share = pieces_ref.shape[0] // out_ref.shape[0]
    for part in range(2):
        for x in range(share):
            block = pieces_ref[pl.ds(part * share + x, share, stride=2 * share), :]
            rows = pl.ds((part * share + x) * share, share)
            for i in range(out_ref.shape[0]):
                out_ref[i, rows, :] = block


def back(blocks, up_ref, down_ref, length):
    turned = product(pair(up_ref), split(blocks))
    rows = turned.shape[1] // length
    points = [parts_across(turned[:, x * length : (x + 1) * length]) for x in range(rows)]
    return product(split(jnp.concatenate(points, axis=0)), pair(down_ref))


def base_kernel(
    me_ref, energy_ref, near_ref, far_ref, orbital_ref, trial_ref, alda_ref, local_ref,
    up_ref, down_ref, out_ref,
):
    length = orbital_ref.shape[2]
    parts = 2 * near_ref.shape[0]
    me = me_ref[0]
    energy = energy_ref[0]
    even = (me & 1) == 0
    scale = 1.0 / float(length * length)
    rows = orbital_ref.shape[1]
    columns = []
    for x in range(rows):
        tiles = []
        for part in range(2):
            for half in range(parts // 2):
                slot = half ^ (me >> 1)
                near = near_ref[slot, part, x]
                far = far_ref[slot, part, x]
                tiles.append(jnp.where(even, near, far))
                tiles.append(jnp.where(even, far, near))
        columns.append(jnp.concatenate(tiles, axis=0))
    value = back(jnp.concatenate(columns, axis=1), up_ref, down_ref, length)
    for x in range(rows):
        factor = orbital_ref[0, x].astype(WIDE) * (alda_ref[x] * scale)
        weight = local_ref[x] - energy
        for k in range(2):
            block = value[x * length : (x + 1) * length, k * length : (k + 1) * length]
            out_ref[k, x] = block * factor + weight * trial_ref[k, 0, x].astype(WIDE)


def field_kernel(potential_ref, orbital_ref, base_ref, up_ref, down_ref, out_ref):
    length = orbital_ref.shape[2]
    parts = potential_ref.shape[0]
    rows = orbital_ref.shape[1]
    columns = []
    for x in range(rows):
        columns.append(
            jnp.concatenate(
                [potential_ref[:, part, x].reshape(length, length) for part in range(2)], axis=0
            )
        )
    value = back(jnp.concatenate(columns, axis=1), up_ref, down_ref, length)
    fields = []
    for x in range(rows):
        orbital = orbital_ref[0, x].astype(WIDE)
        for k in range(2):
            block = value[x * length : (x + 1) * length, k * length : (k + 1) * length]
            fields.append(block * orbital + base_ref[k, x])
    table = (up_ref[0, :length, :], up_ref[1, :length, :])
    turned = product(split(jnp.concatenate(fields, axis=0)), table)
    for x in range(rows):
        points = swap_blocks(turned[2 * x * length : 2 * (x + 1) * length])
        waves = product(pair(down_ref), split(points))
        for k in range(2):
            for part in range(2):
                block = waves[part * length : (part + 1) * length, k * length : (k + 1) * length]
                out_ref[:, k, part, x] = block.reshape(parts, length // parts, length)


def final_kernel(pieces_ref, x_ref, real_ref, imag_ref):
    length = real_ref.shape[-1]
    share = real_ref.shape[2]
    table = pair(x_ref)
    for k in range(2):
        for b in range(share):
            parts = []
            for part in range(2):
                start = (k * 2 + part) * share * share + b
                block = pieces_ref[:, pl.ds(start, share, stride=share), :]
                parts.append(block.reshape(length, length))
            turned = product(split(jnp.concatenate(parts, axis=0).T), table)
            real_ref[k, 0, b] = turned[:, :length]
            imag_ref[k, 0, b] = turned[:, length:]


def signed(positions, length):
    return jnp.where(2 * positions < length, positions, positions - length).astype(WIDE)


def line_coulomb(b, length):
    a = lax.broadcasted_iota(jnp.int32, (length, length), 0)
    c = lax.broadcasted_iota(jnp.int32, (length, length), 1)
    squared = signed(a, length) ** 2 + signed(b, length) ** 2 + signed(c, length) ** 2
    scaled = box_length**2 / math.pi / jnp.maximum(squared, 1.0)
    return jnp.where(squared > 0, scaled, 0.0) / float(length**3)


def call(body, shapes, grant=GRANT, **options):
    return pl.pallas_call(
        body,
        out_shape=jax.tree.map(
            lambda s: jax.ShapeDtypeStruct(s, WIDE),
            shapes,
            is_leaf=lambda s: isinstance(s, tuple) and isinstance(s[0], int),
        ),
        compiler_params=pltpu.CompilerParams(vmem_limit_bytes=grant),
        **options,
    )


def exchange(array, axis):
    return lax.all_to_all(array, axis, split_axis=0, concat_axis=0, tiled=True)


def partner(array, mask):
    return lax.ppermute(array, "band", [(i, i ^ mask) for i in range(lax.axis_size("band"))])


def per_device(orbitals, trials, alda_kernel, local_potential, band_energies):
    length = orbitals.shape[2]
    parts = lax.axis_size("band")
    share = length // parts
    points = share * share
    tables = {name: jnp.asarray(table) for name, table in make_tables(length).items()}
    me = lax.axis_index("band")
    place = lax.axis_index("grid")
    copies = parts // share
    kernel = line_coulomb(me * share + place // copies, length)
    own_up = lax.dynamic_slice_in_dim(tables["up"], (place % copies) * length, length, 1)

    scalar = pl.BlockSpec(memory_space=pltpu.SMEM)
    orbital_block = pl.BlockSpec((1, ROWS, length, length), lambda i: (0, i, 0, 0))
    trial_block = pl.BlockSpec((2, 1, ROWS, length, length), lambda i: (0, 0, i, 0, 0))
    table_block = pl.BlockSpec((2, 2 * length, 2 * length), lambda i: (0, 0, 0))
    share_block = pl.BlockSpec((parts, 2, ROWS, share, length), lambda i: (0, 0, i, 0, 0))
    half_block = pl.BlockSpec((parts // 2, 2, ROWS, share, length), lambda i: (0, 0, i, 0, 0))
    local_block = pl.BlockSpec((ROWS, length, length), lambda i: (i, 0, 0))
    base_block = pl.BlockSpec((2, ROWS, length, length), lambda i: (0, i, 0, 0))
    steps = (share // ROWS,)

    held = pl.BlockSpec(memory_space=pltpu.HBM)
    shape = (parts, 2, share, share, length)
    pieces = call(
        density_kernel,
        shape,
        grant=WIDE_GRANT,
        in_specs=[held] * 4,
        out_specs=held,
        scratch_shapes=[
            pltpu.VMEM(orbitals.shape, NARROW),
            pltpu.VMEM(trials.shape, NARROW),
            pltpu.VMEM(tables["up"].shape, NARROW),
            pltpu.VMEM(tables["down"].shape, NARROW),
            pltpu.VMEM(shape, WIDE),
            pltpu.SemaphoreType.DMA((2,)),
            pltpu.SemaphoreType.DMA((2, 2)),
            pltpu.SemaphoreType.DMA((2,)),
        ],
    )(orbitals, trials, tables["up"], tables["down"])
    pieces = exchange(pieces.reshape(parts, 2 * points, length), "band")
    spectrum, lines = call(share_kernel, [(2 * points, length), (parts, 2 * share, length)])(pieces)
    lines = exchange(lines, "grid")
    held = {0: spectrum}
    for mask in (2, 4, 8):
        held[mask] = partner(spectrum, mask)
    lines = call(line_kernel, (parts, share, length))(
        lines, kernel, tables["down"], own_up
    )
    lines, held[2], held[4], held[8] = lax.optimization_barrier((lines, held[2], held[4], held[8]))
    lines = exchange(lines, "grid").reshape(parts * share, length)
    both = partner(jnp.stack([held[4], held[8]]), 2)
    held[6], held[10] = both[0], both[1]
    held[12] = partner(held[8], 4)
    held[14] = partner(spectrum, 14)
    away = {}
    for masks in ((0, 2, 4, 8), (6, 10, 12, 14)):
        group = partner(jnp.stack([held[mask] for mask in masks]), 1)
        for i, mask in enumerate(masks):
            away[mask] = group[i]
    near = jnp.stack([held[mask] for mask in range(0, parts, 2)])
    far = jnp.stack([away[mask] for mask in range(0, parts, 2)])
    potential = call(spread_kernel, (parts, 2 * points, length))(lines)
    potential = exchange(potential, "band").reshape(parts, 2, share, share, length)
    base = call(
        base_kernel,
        (2, share, length, length),
        grid=steps,
        in_specs=[
            scalar, scalar, half_block, half_block, orbital_block, trial_block,
            local_block, local_block, table_block, table_block,
        ],
        out_specs=base_block,
    )(
        me.reshape(1),
        band_energies,
        near.reshape(parts // 2, 2, share, share, length),
        far.reshape(parts // 2, 2, share, share, length),
        orbitals,
        trials,
        alda_kernel,
        local_potential,
        tables["up"],
        tables["down"],
    )
    fields = call(
        field_kernel,
        (parts, 2, 2, share, share, length),
        grid=steps,
        in_specs=[share_block, orbital_block, base_block, table_block, table_block],
        out_specs=pl.BlockSpec(
            (parts, 2, 2, ROWS, share, length), lambda i: (0, 0, 0, i, 0, 0)
        ),
    )(potential, orbitals, base, tables["up"], tables["down"])
    received = exchange(fields.reshape(parts, 4 * points, length), "grid")
    shape = (2, 1, share, length, length)
    return tuple(call(final_kernel, [shape, shape])(received, tables["last"]))


def solution(mesh):
    placed = (
        P("band", "grid", None, None),
        P(None, "band", "grid", None, None),
        P("grid", None, None),
        P("grid", None, None),
        P("band"),
    )

    return jax.shard_map(
        per_device,
        mesh=mesh,
        in_specs=placed,
        out_specs=(P(None, "band", "grid", None, None), P(None, "band", "grid", None, None)),
        check_vma=False,
    )
```

```python
import functools
import math

import jax
import jax.numpy as jnp
import numpy as np
from jax import lax
from jax.experimental import pallas as pl
from jax.experimental.pallas import tpu as pltpu
from jax.sharding import PartitionSpec as P


box_length = 30.0
NARROW = jnp.bfloat16
WIDE = jnp.float32
ROWS = 8
GRANT = 20 * 2**20
WIDE_GRANT = 60 * 2**20


def halves(table):
    high = table.astype(np.float32).astype(jnp.bfloat16)
    low = (table - high.astype(np.float64)).astype(np.float32).astype(jnp.bfloat16)
    return np.stack([high, low])


@functools.cache
def make_tables(length):
    wrapped = np.outer(np.arange(length), np.arange(length)) % length
    angles = wrapped.astype(np.float64) * (2.0 * math.pi / length)
    cosine, sine = np.cos(angles), np.sin(angles)
    return {
        "down": halves(np.block([[cosine, sine], [-sine, cosine]])),
        "up": halves(np.block([[cosine, -sine], [sine, cosine]])),
        "last": halves(np.block([[cosine, -sine], [sine, cosine]]) * float(length) ** -1.5),
    }


def split(value):
    high = value.astype(NARROW)
    return high, (value - high.astype(WIDE)).astype(NARROW)


def mul(left, right):
    return lax.dot_general(left, right, (((1,), (0,)), ((), ())), preferred_element_type=WIDE)


def product(left, right):
    left_high, left_low = left
    right_high, right_low = right
    return mul(left_high, right_high) + mul(left_low, right_high) + mul(left_high, right_low)


def pair(ref):
    return ref[0], ref[1]


def swap_blocks(value):
    rows, columns = value.shape[0] // 2, value.shape[1] // 2
    left = jnp.concatenate([value[:rows, :columns], value[rows:, :columns]], axis=1)
    right = jnp.concatenate([value[:rows, columns:], value[rows:, columns:]], axis=1)
    return jnp.concatenate([left, right], axis=0)


def parts_down(value):
    half = value.shape[1] // 2
    return jnp.concatenate([value[:, :half], value[:, half:]], axis=0)


def parts_across(value):
    half = value.shape[0] // 2
    return jnp.concatenate([value[:half], value[half:]], axis=1)


def density_kernel(me_ref, orbital_in, trial_in, up_in, down_in, *refs):
    (
        kept_hbm, near_hbm, out_hbm, orbital_ref, trial_ref, up_ref, down_ref, mixed_ref, out_ref,
        table_sems, row_sems, out_sems,
    ) = refs
    me = me_ref[0]
    length = orbital_ref.shape[2]
    parts, share = out_ref.shape[0], out_ref.shape[3]
    half = orbital_ref.shape[1] // 2
    tables = [
        pltpu.make_async_copy(up_in, up_ref, table_sems.at[0]),
        pltpu.make_async_copy(down_in, down_ref, table_sems.at[1]),
    ]
    rows = [pl.ds(i * half, half) for i in range(2)]
    orbitals, trials = [], []
    for i in range(2):
        part = (slice(None), rows[i])
        orbitals.append(
            pltpu.make_async_copy(orbital_in.at[part], orbital_ref.at[part], row_sems.at[i, 0])
        )
        part = (slice(None), slice(None), rows[i])
        trials.append(
            pltpu.make_async_copy(trial_in.at[part], trial_ref.at[part], row_sems.at[i, 1])
        )
    outs = [
        [
            pltpu.make_async_copy(mixed_ref.at[1], near_hbm, out_sems.at[1]),
            pltpu.make_async_copy(mixed_ref.at[0], kept_hbm, out_sems.at[0]),
        ],
        [pltpu.make_async_copy(out_ref, out_hbm, out_sems.at[2])],
    ]
    for copy in (tables[0], orbitals[0], trials[0], tables[1], orbitals[1], trials[1]):
        copy.start()
    for copy in tables:
        copy.wait()
    for i in range(2):
        orbitals[i].wait()
        trials[i].wait()
        values = []
        for x in range(half):
            orbital = 2.0 * orbital_ref[0, i * half + x].astype(WIDE)
            values.append(
                jnp.concatenate(
                    [trial_ref[k, 0, i * half + x].astype(WIDE) * orbital for k in range(2)], axis=1
                )
            )
        turned = product(split(jnp.concatenate(values, axis=0)), pair(up_ref))
        columns = [parts_down(turned[x * length : (x + 1) * length]) for x in range(half)]
        turned = product(pair(down_ref), split(jnp.concatenate(columns, axis=1)))
        for x in range(half):
            for part in range(2):
                block = turned[part * length : (part + 1) * length, x * length : (x + 1) * length]
                if i == 1:
                    out_ref[:, part, x] = block.reshape(parts, share, length)
                    continue
                for n in range(parts):
                    tile = block[n * share : (n + 1) * share]
                    mixed_ref[(n ^ me) & 1, (n ^ me) >> 1, part, x] = tile
        for copy in outs[i]:
            copy.start()
    for copy in outs[0] + outs[1]:
        copy.wait()


def share_kernel(pieces_ref, *refs):
    *near_refs, share_ref, out_ref = refs
    first = near_refs[0][...]
    for ref in near_refs[1:]:
        first = first + ref[...]
    second = pieces_ref[0]
    for i in range(1, pieces_ref.shape[0]):
        second = second + pieces_ref[i]
    rows = first.shape[0] // 2
    for part in range(2):
        held = slice(part * rows, (part + 1) * rows)
        share_ref[2 * part * rows : (2 * part + 1) * rows, :] = first[held]
        share_ref[(2 * part + 1) * rows : 2 * (part + 1) * rows, :] = second[held]
    copies, rows, _ = out_ref.shape
    share = rows // 2
    for b in range(share):
        block = share_ref[pl.ds(b, rows, stride=share), :]
        for i in range(copies // share):
            out_ref[b * (copies // share) + i] = block


def line_kernel(pieces_ref, kernel_ref, down_ref, up_ref, out_ref):
    parts, rows, length = pieces_ref.shape
    share = rows // 2
    columns = jnp.concatenate(
        [pieces_ref[:, :share, :].reshape(length, length), pieces_ref[:, share:, :].reshape(length, length)],
        axis=0,
    )
    turned = product(pair(down_ref), split(columns))
    kernel = kernel_ref[...]
    turned = turned * jnp.concatenate([kernel, kernel], axis=0)
    out_ref[...] = product(pair(up_ref), split(turned)).reshape(parts, share, length)


def turn_kernel(pieces_ref, out_ref):
    share = math.isqrt(out_ref.shape[0] // 2)
    for part in range(2):
        for x in range(share):
            block = pieces_ref[pl.ds(part * share + x, share, stride=2 * share), :]
            out_ref[pl.ds((part * share + x) * share, share), :] = block


def all_columns(me, near_ref, far_ref, x):
    even = (me & 1) == 0
    tiles = []
    for part in range(2):
        for half in range(near_ref.shape[0]):
            slot = half ^ (me >> 1)
            near = near_ref[slot, part, x]
            far = far_ref[slot, part, x]
            tiles.append(jnp.where(even, near, far))
            tiles.append(jnp.where(even, far, near))
    return jnp.concatenate(tiles, axis=0)


def back(blocks, up_ref, down_ref, length):
    turned = product(pair(up_ref), split(blocks))
    rows = turned.shape[1] // length
    points = [parts_across(turned[:, x * length : (x + 1) * length]) for x in range(rows)]
    return product(split(jnp.concatenate(points, axis=0)), pair(down_ref))


def base_kernel(
    me_ref, energy_ref, near_ref, far_ref, orbital_ref, trial_ref, alda_ref, local_ref,
    up_ref, down_ref, out_ref,
):
    length = orbital_ref.shape[2]
    me = me_ref[0]
    energy = energy_ref[0]
    scale = 1.0 / float(length * length)
    rows = orbital_ref.shape[1]
    columns = [all_columns(me, near_ref, far_ref, x) for x in range(rows)]
    value = back(jnp.concatenate(columns, axis=1), up_ref, down_ref, length)
    for x in range(rows):
        factor = orbital_ref[0, x].astype(WIDE) * (alda_ref[x] * scale)
        weight = local_ref[x] - energy
        for k in range(2):
            block = value[x * length : (x + 1) * length, k * length : (k + 1) * length]
            out_ref[k, x] = block * factor + weight * trial_ref[k, 0, x].astype(WIDE)


def field_kernel(me_ref, *refs):
    *share_refs, orbital_ref, base_ref, up_ref, down_ref, out_ref, near_ref, far_ref = refs
    count = near_ref.shape[0]
    for i in range(count):
        near_ref[i] = share_refs[i][...]
    start = 0
    for ref in share_refs[count:]:
        far_ref[start : start + ref.shape[0]] = ref[...]
        start += ref.shape[0]
    length = orbital_ref.shape[2]
    parts = out_ref.shape[0]
    rows = orbital_ref.shape[1]
    columns = [all_columns(me_ref[0], near_ref, far_ref, x) for x in range(rows)]
    value = back(jnp.concatenate(columns, axis=1), up_ref, down_ref, length)
    fields = []
    for x in range(rows):
        orbital = orbital_ref[0, x].astype(WIDE)
        for k in range(2):
            block = value[x * length : (x + 1) * length, k * length : (k + 1) * length]
            fields.append(block * orbital + base_ref[k, x])
    table = (up_ref[0, :length, :], up_ref[1, :length, :])
    turned = product(split(jnp.concatenate(fields, axis=0)), table)
    for x in range(rows):
        points = swap_blocks(turned[2 * x * length : 2 * (x + 1) * length])
        waves = product(pair(down_ref), split(points))
        for k in range(2):
            for part in range(2):
                block = waves[part * length : (part + 1) * length, k * length : (k + 1) * length]
                out_ref[:, k, part, x] = block.reshape(parts, length // parts, length)


def final_kernel(pieces_ref, x_ref, real_ref, imag_ref):
    length = real_ref.shape[-1]
    share = real_ref.shape[2]
    table = pair(x_ref)
    for k in range(2):
        for b in range(share):
            parts = []
            for part in range(2):
                start = (k * 2 + part) * share * share + b
                block = pieces_ref[:, pl.ds(start, share, stride=share), :]
                parts.append(block.reshape(length, length))
            turned = product(split(jnp.concatenate(parts, axis=0).T), table)
            real_ref[k, 0, b] = turned[:, :length]
            imag_ref[k, 0, b] = turned[:, length:]


def signed(positions, length):
    return jnp.where(2 * positions < length, positions, positions - length).astype(WIDE)


def line_coulomb(b, length):
    a = lax.broadcasted_iota(jnp.int32, (length, length), 0)
    c = lax.broadcasted_iota(jnp.int32, (length, length), 1)
    squared = signed(a, length) ** 2 + signed(b, length) ** 2 + signed(c, length) ** 2
    scaled = box_length**2 / math.pi / jnp.maximum(squared, 1.0)
    return jnp.where(squared > 0, scaled, 0.0) / float(length**3)


def call(body, shapes, grant=GRANT, **options):
    return pl.pallas_call(
        body,
        out_shape=jax.tree.map(
            lambda s: jax.ShapeDtypeStruct(s, WIDE),
            shapes,
            is_leaf=lambda s: isinstance(s, tuple) and isinstance(s[0], int),
        ),
        compiler_params=pltpu.CompilerParams(vmem_limit_bytes=grant),
        **options,
    )


def exchange(array, axis):
    return lax.all_to_all(array, axis, split_axis=0, concat_axis=0, tiled=True)


def partner(array, mask):
    return lax.ppermute(array, "band", [(i, i ^ mask) for i in range(lax.axis_size("band"))])


def per_device(orbitals, trials, alda_kernel, local_potential, band_energies):
    length = orbitals.shape[2]
    parts = lax.axis_size("band")
    share = length // parts
    points = share * share
    tables = {name: jnp.asarray(table) for name, table in make_tables(length).items()}
    me = lax.axis_index("band")
    place = lax.axis_index("grid")
    copies = parts // share
    kernel = line_coulomb(me * share + place // copies, length)
    own_up = lax.dynamic_slice_in_dim(tables["up"], (place % copies) * length, length, 1)

    scalar = pl.BlockSpec(memory_space=pltpu.SMEM)
    orbital_block = pl.BlockSpec((1, ROWS, length, length), lambda i: (0, i, 0, 0))
    trial_block = pl.BlockSpec((2, 1, ROWS, length, length), lambda i: (0, 0, i, 0, 0))
    table_block = pl.BlockSpec((2, 2 * length, 2 * length), lambda i: (0, 0, 0))
    half_block = pl.BlockSpec((parts // 2, 2, ROWS, share, length), lambda i: (0, 0, i, 0, 0))
    local_block = pl.BlockSpec((ROWS, length, length), lambda i: (i, 0, 0))
    base_block = pl.BlockSpec((2, ROWS, length, length), lambda i: (0, i, 0, 0))
    steps = (share // ROWS,)

    held = pl.BlockSpec(memory_space=pltpu.HBM)
    half = share // 2
    some = (parts // 2, 2, half, share, length)
    kept, near, pieces = call(
        density_kernel,
        [some, some, (parts, 2, half, share, length)],
        grant=WIDE_GRANT,
        in_specs=[scalar] + [held] * 4,
        out_specs=[held] * 3,
        scratch_shapes=[
            pltpu.VMEM(orbitals.shape, NARROW),
            pltpu.VMEM(trials.shape, NARROW),
            pltpu.VMEM(tables["up"].shape, NARROW),
            pltpu.VMEM(tables["down"].shape, NARROW),
            pltpu.VMEM((2, *some), WIDE),
            pltpu.VMEM((parts, 2, half, share, length), WIDE),
            pltpu.SemaphoreType.DMA((2,)),
            pltpu.SemaphoreType.DMA((2, 2)),
            pltpu.SemaphoreType.DMA((3,)),
        ],
    )(me.reshape(1), orbitals, trials, tables["up"], tables["down"])
    near = partner(near.reshape(parts // 2, points, length), 1)
    near = near + kept.reshape(parts // 2, points, length)
    near = [near[0]] + [partner(near[i], 2 * i) for i in range(1, parts // 2)]
    pieces = exchange(pieces.reshape(parts, points, length), "band")
    spectrum, lines = call(
        share_kernel, [(2 * points, length), (parts, 2 * share, length)]
    )(pieces, *near)
    lines = exchange(lines, "grid")
    held = {0: spectrum}
    for mask in (2, 4, 8):
        held[mask] = partner(spectrum, mask)
    lines = call(line_kernel, (parts, share, length))(
        lines, kernel, tables["down"], own_up
    )
    lines, held[2], held[4], held[8] = lax.optimization_barrier((lines, held[2], held[4], held[8]))
    lines = exchange(lines, "grid").reshape(parts * share, length)
    both = partner(jnp.stack([held[4], held[8]]), 2)
    held[6], held[10] = both[0], both[1]
    held[12] = partner(held[8], 4)
    held[14] = partner(spectrum, 14)
    away = {}
    for masks in ((0, 2, 4, 8), (6, 10, 12, 14)):
        group = partner(jnp.stack([held[mask] for mask in masks]), 1)
        for i, mask in enumerate(masks):
            away[mask] = group[i]
    near = jnp.stack([held[mask] for mask in range(0, parts, 2)])
    far = jnp.stack([away[mask] for mask in range(0, parts, 2)])
    own = call(turn_kernel, (2 * points, length))(lines)
    gained = {0: own}
    for masks in ((2, 4, 6), (8, 10), (12, 14)):
        for mask in masks:
            gained[mask] = partner(own, mask)
    passed = [
        partner(jnp.stack([gained[mask] for mask in masks]), 1)
        for masks in ((0, 2, 4, 6), (8, 10), (12, 14))
    ]
    spread = [gained[mask].reshape(2, share, share, length) for mask in range(0, parts, 2)]
    spread += [array.reshape(-1, 2, share, share, length) for array in passed]
    base = call(
        base_kernel,
        (2, share, length, length),
        grid=steps,
        in_specs=[
            scalar, scalar, half_block, half_block, orbital_block, trial_block,
            local_block, local_block, table_block, table_block,
        ],
        out_specs=base_block,
    )(
        me.reshape(1),
        band_energies,
        near.reshape(parts // 2, 2, share, share, length),
        far.reshape(parts // 2, 2, share, share, length),
        orbitals,
        trials,
        alda_kernel,
        local_potential,
        tables["up"],
        tables["down"],
    )
    vector = pl.BlockSpec(memory_space=pltpu.VMEM)
    held = pltpu.VMEM((parts // 2, 2, share, share, length), WIDE)
    fields = call(
        field_kernel,
        (parts, 2, 2, share, share, length),
        in_specs=[scalar] + [vector] * (len(spread) + 4),
        scratch_shapes=[held, held],
    )(me.reshape(1), *spread, orbitals, base, tables["up"], tables["down"])
    received = exchange(fields.reshape(parts, 4 * points, length), "grid")
    shape = (2, 1, share, length, length)
    return tuple(call(final_kernel, [shape, shape])(received, tables["last"]))


def solution(mesh):
    placed = (
        P("band", "grid", None, None),
        P(None, "band", "grid", None, None),
        P("grid", None, None),
        P("grid", None, None),
        P("band"),
    )

    return jax.shard_map(
        per_device,
        mesh=mesh,
        in_specs=placed,
        out_specs=(P(None, "band", "grid", None, None), P(None, "band", "grid", None, None)),
        check_vma=False,
    )
```

```python
import functools
import math

import jax
import jax.numpy as jnp
import numpy as np
from jax import lax
from jax.experimental import pallas as pl
from jax.experimental.pallas import tpu as pltpu
from jax.sharding import PartitionSpec as P


box_length = 30.0
NARROW = jnp.bfloat16
WIDE = jnp.float32
ROWS = 8
GRANT = 20 * 2**20
WIDE_GRANT = 60 * 2**20


def halves(table):
    high = table.astype(np.float32).astype(jnp.bfloat16)
    low = (table - high.astype(np.float64)).astype(np.float32).astype(jnp.bfloat16)
    return np.stack([high, low])


@functools.cache
def make_tables(length):
    wrapped = np.outer(np.arange(length), np.arange(length)) % length
    angles = wrapped.astype(np.float64) * (2.0 * math.pi / length)
    cosine, sine = np.cos(angles), np.sin(angles)
    return {
        "down": halves(np.block([[cosine, sine], [-sine, cosine]])),
        "up": halves(np.block([[cosine, -sine], [sine, cosine]])),
        "last": halves(np.block([[cosine, -sine], [sine, cosine]]) * float(length) ** -1.5),
    }


def split(value):
    high = value.astype(NARROW)
    return high, (value - high.astype(WIDE)).astype(NARROW)


def mul(left, right):
    return lax.dot_general(left, right, (((1,), (0,)), ((), ())), preferred_element_type=WIDE)


def product(left, right):
    left_high, left_low = left
    right_high, right_low = right
    return mul(left_high, right_high) + mul(left_low, right_high) + mul(left_high, right_low)


def pair(ref):
    return ref[0], ref[1]


def swap_blocks(value):
    rows, columns = value.shape[0] // 2, value.shape[1] // 2
    left = jnp.concatenate([value[:rows, :columns], value[rows:, :columns]], axis=1)
    right = jnp.concatenate([value[:rows, columns:], value[rows:, columns:]], axis=1)
    return jnp.concatenate([left, right], axis=0)


def parts_down(value):
    half = value.shape[1] // 2
    return jnp.concatenate([value[:, :half], value[:, half:]], axis=0)


def parts_across(value):
    half = value.shape[0] // 2
    return jnp.concatenate([value[:half], value[half:]], axis=1)


def density_kernel(me_ref, orbital_in, trial_in, up_in, down_in, *refs):
    (
        kept_hbm, near_hbm, out_hbm, orbital_ref, trial_ref, up_ref, down_ref, mixed_ref, out_ref,
        table_sems, row_sems, out_sems,
    ) = refs
    me = me_ref[0]
    length = orbital_ref.shape[2]
    parts, share = out_ref.shape[0], out_ref.shape[3]
    half = orbital_ref.shape[1] // 2
    tables = [
        pltpu.make_async_copy(up_in, up_ref, table_sems.at[0]),
        pltpu.make_async_copy(down_in, down_ref, table_sems.at[1]),
    ]
    rows = [pl.ds(i * half, half) for i in range(2)]
    orbitals, trials = [], []
    for i in range(2):
        part = (slice(None), rows[i])
        orbitals.append(
            pltpu.make_async_copy(orbital_in.at[part], orbital_ref.at[part], row_sems.at[i, 0])
        )
        part = (slice(None), slice(None), rows[i])
        trials.append(
            pltpu.make_async_copy(trial_in.at[part], trial_ref.at[part], row_sems.at[i, 1])
        )
    outs = [
        [
            pltpu.make_async_copy(mixed_ref.at[1], near_hbm, out_sems.at[1]),
            pltpu.make_async_copy(mixed_ref.at[0], kept_hbm, out_sems.at[0]),
        ],
        [pltpu.make_async_copy(out_ref, out_hbm, out_sems.at[2])],
    ]
    for copy in (tables[0], orbitals[0], trials[0], tables[1], orbitals[1], trials[1]):
        copy.start()
    for copy in tables:
        copy.wait()
    for i in range(2):
        orbitals[i].wait()
        trials[i].wait()
        values = []
        for x in range(half):
            orbital = 2.0 * orbital_ref[0, i * half + x].astype(WIDE)
            values.append(
                jnp.concatenate(
                    [trial_ref[k, 0, i * half + x].astype(WIDE) * orbital for k in range(2)], axis=1
                )
            )
        turned = product(split(jnp.concatenate(values, axis=0)), pair(up_ref))
        columns = [parts_down(turned[x * length : (x + 1) * length]) for x in range(half)]
        turned = product(pair(down_ref), split(jnp.concatenate(columns, axis=1)))
        for x in range(half):
            for part in range(2):
                block = turned[part * length : (part + 1) * length, x * length : (x + 1) * length]
                if i == 1:
                    out_ref[:, part, x] = block.reshape(parts, share, length)
                    continue
                for n in range(parts):
                    tile = block[n * share : (n + 1) * share]
                    mixed_ref[(n ^ me) & 1, (n ^ me) >> 1, part, x] = tile
        for copy in outs[i]:
            copy.start()
    for copy in outs[0] + outs[1]:
        copy.wait()


def share_kernel(pieces_ref, *refs):
    *near_refs, share_ref, out_ref = refs
    first = near_refs[0][...]
    for ref in near_refs[1:]:
        first = first + ref[...]
    second = pieces_ref[0]
    for i in range(1, pieces_ref.shape[0]):
        second = second + pieces_ref[i]
    rows = first.shape[0] // 2
    for part in range(2):
        held = slice(part * rows, (part + 1) * rows)
        share_ref[2 * part * rows : (2 * part + 1) * rows, :] = first[held]
        share_ref[(2 * part + 1) * rows : 2 * (part + 1) * rows, :] = second[held]
    copies, rows, _ = out_ref.shape
    share = rows // 2
    for b in range(share):
        block = share_ref[pl.ds(b, rows, stride=share), :]
        for i in range(copies // share):
            out_ref[b * (copies // share) + i] = block


def line_kernel(pieces_ref, kernel_ref, down_ref, up_ref, out_ref):
    parts, rows, length = pieces_ref.shape
    share = rows // 2
    columns = jnp.concatenate(
        [pieces_ref[:, :share, :].reshape(length, length), pieces_ref[:, share:, :].reshape(length, length)],
        axis=0,
    )
    turned = product(pair(down_ref), split(columns))
    kernel = kernel_ref[...]
    turned = turned * jnp.concatenate([kernel, kernel], axis=0)
    out_ref[...] = product(pair(up_ref), split(turned)).reshape(parts, share, length)


def spread_kernel(pieces_ref, out_ref):
    share = pieces_ref.shape[0] // out_ref.shape[0]
    for part in range(2):
        for x in range(share):
            block = pieces_ref[pl.ds(part * share + x, share, stride=2 * share), :]
            rows = pl.ds((part * share + x) * share, share)
            for i in range(out_ref.shape[0]):
                out_ref[i, rows, :] = block


def back(blocks, up_ref, down_ref, length):
    turned = product(pair(up_ref), split(blocks))
    rows = turned.shape[1] // length
    points = [parts_across(turned[:, x * length : (x + 1) * length]) for x in range(rows)]
    return product(split(jnp.concatenate(points, axis=0)), pair(down_ref))


def base_kernel(
    me_ref, energy_ref, near_ref, far_ref, orbital_ref, trial_ref, alda_ref, local_ref,
    up_ref, down_ref, out_ref,
):
    length = orbital_ref.shape[2]
    parts = 2 * near_ref.shape[0]
    me = me_ref[0]
    energy = energy_ref[0]
    even = (me & 1) == 0
    scale = 1.0 / float(length * length)
    rows = orbital_ref.shape[1]
    columns = []
    for x in range(rows):
        tiles = []
        for part in range(2):
            for half in range(parts // 2):
                slot = half ^ (me >> 1)
                near = near_ref[slot, part, x]
                far = far_ref[slot, part, x]
                tiles.append(jnp.where(even, near, far))
                tiles.append(jnp.where(even, far, near))
        columns.append(jnp.concatenate(tiles, axis=0))
    value = back(jnp.concatenate(columns, axis=1), up_ref, down_ref, length)
    for x in range(rows):
        factor = orbital_ref[0, x].astype(WIDE) * (alda_ref[x] * scale)
        weight = local_ref[x] - energy
        for k in range(2):
            block = value[x * length : (x + 1) * length, k * length : (k + 1) * length]
            out_ref[k, x] = block * factor + weight * trial_ref[k, 0, x].astype(WIDE)


def field_kernel(potential_ref, orbital_ref, base_ref, up_ref, down_ref, out_ref):
    length = orbital_ref.shape[2]
    parts = potential_ref.shape[0]
    rows = orbital_ref.shape[1]
    columns = []
    for x in range(rows):
        columns.append(
            jnp.concatenate(
                [potential_ref[:, part, x].reshape(length, length) for part in range(2)], axis=0
            )
        )
    value = back(jnp.concatenate(columns, axis=1), up_ref, down_ref, length)
    fields = []
    for x in range(rows):
        orbital = orbital_ref[0, x].astype(WIDE)
        for k in range(2):
            block = value[x * length : (x + 1) * length, k * length : (k + 1) * length]
            fields.append(block * orbital + base_ref[k, x])
    table = (up_ref[0, :length, :], up_ref[1, :length, :])
    turned = product(split(jnp.concatenate(fields, axis=0)), table)
    for x in range(rows):
        points = swap_blocks(turned[2 * x * length : 2 * (x + 1) * length])
        waves = product(pair(down_ref), split(points))
        for k in range(2):
            for part in range(2):
                block = waves[part * length : (part + 1) * length, k * length : (k + 1) * length]
                out_ref[:, k, part, x] = block.reshape(parts, length // parts, length)


def final_kernel(pieces_ref, x_ref, real_ref, imag_ref):
    length = real_ref.shape[-1]
    share = real_ref.shape[2]
    table = pair(x_ref)
    for k in range(2):
        for b in range(share):
            parts = []
            for part in range(2):
                start = (k * 2 + part) * share * share + b
                block = pieces_ref[:, pl.ds(start, share, stride=share), :]
                parts.append(block.reshape(length, length))
            turned = product(split(jnp.concatenate(parts, axis=0).T), table)
            real_ref[k, 0, b] = turned[:, :length]
            imag_ref[k, 0, b] = turned[:, length:]


def signed(positions, length):
    return jnp.where(2 * positions < length, positions, positions - length).astype(WIDE)


def line_coulomb(b, length):
    a = lax.broadcasted_iota(jnp.int32, (length, length), 0)
    c = lax.broadcasted_iota(jnp.int32, (length, length), 1)
    squared = signed(a, length) ** 2 + signed(b, length) ** 2 + signed(c, length) ** 2
    scaled = box_length**2 / math.pi / jnp.maximum(squared, 1.0)
    return jnp.where(squared > 0, scaled, 0.0) / float(length**3)


def call(body, shapes, grant=GRANT, **options):
    return pl.pallas_call(
        body,
        out_shape=jax.tree.map(
            lambda s: jax.ShapeDtypeStruct(s, WIDE),
            shapes,
            is_leaf=lambda s: isinstance(s, tuple) and isinstance(s[0], int),
        ),
        compiler_params=pltpu.CompilerParams(vmem_limit_bytes=grant),
        **options,
    )


def exchange(array, axis):
    return lax.all_to_all(array, axis, split_axis=0, concat_axis=0, tiled=True)


def partner(array, mask):
    return lax.ppermute(array, "band", [(i, i ^ mask) for i in range(lax.axis_size("band"))])


def per_device(orbitals, trials, alda_kernel, local_potential, band_energies):
    length = orbitals.shape[2]
    parts = lax.axis_size("band")
    share = length // parts
    points = share * share
    tables = {name: jnp.asarray(table) for name, table in make_tables(length).items()}
    me = lax.axis_index("band")
    place = lax.axis_index("grid")
    copies = parts // share
    kernel = line_coulomb(me * share + place // copies, length)
    own_up = lax.dynamic_slice_in_dim(tables["up"], (place % copies) * length, length, 1)

    scalar = pl.BlockSpec(memory_space=pltpu.SMEM)
    orbital_block = pl.BlockSpec((1, ROWS, length, length), lambda i: (0, i, 0, 0))
    trial_block = pl.BlockSpec((2, 1, ROWS, length, length), lambda i: (0, 0, i, 0, 0))
    table_block = pl.BlockSpec((2, 2 * length, 2 * length), lambda i: (0, 0, 0))
    share_block = pl.BlockSpec((parts, 2, ROWS, share, length), lambda i: (0, 0, i, 0, 0))
    half_block = pl.BlockSpec((parts // 2, 2, ROWS, share, length), lambda i: (0, 0, i, 0, 0))
    local_block = pl.BlockSpec((ROWS, length, length), lambda i: (i, 0, 0))
    base_block = pl.BlockSpec((2, ROWS, length, length), lambda i: (0, i, 0, 0))
    steps = (share // ROWS,)

    held = pl.BlockSpec(memory_space=pltpu.HBM)
    half = share // 2
    some = (parts // 2, 2, half, share, length)
    kept, near, pieces = call(
        density_kernel,
        [some, some, (parts, 2, half, share, length)],
        grant=WIDE_GRANT,
        in_specs=[scalar] + [held] * 4,
        out_specs=[held] * 3,
        scratch_shapes=[
            pltpu.VMEM(orbitals.shape, NARROW),
            pltpu.VMEM(trials.shape, NARROW),
            pltpu.VMEM(tables["up"].shape, NARROW),
            pltpu.VMEM(tables["down"].shape, NARROW),
            pltpu.VMEM((2, *some), WIDE),
            pltpu.VMEM((parts, 2, half, share, length), WIDE),
            pltpu.SemaphoreType.DMA((2,)),
            pltpu.SemaphoreType.DMA((2, 2)),
            pltpu.SemaphoreType.DMA((3,)),
        ],
    )(me.reshape(1), orbitals, trials, tables["up"], tables["down"])
    near = partner(near.reshape(parts // 2, points, length), 1)
    near = near + kept.reshape(parts // 2, points, length)
    near = [near[0]] + [partner(near[i], 2 * i) for i in range(1, parts // 2)]
    pieces = exchange(pieces.reshape(parts, points, length), "band")
    spectrum, lines = call(
        share_kernel, [(2 * points, length), (parts, 2 * share, length)]
    )(pieces, *near)
    lines = exchange(lines, "grid")
    held = {0: spectrum}
    for mask in (2, 4, 8):
        held[mask] = partner(spectrum, mask)
    lines = call(line_kernel, (parts, share, length))(
        lines, kernel, tables["down"], own_up
    )
    _, held[2], held[4], held[8] = lax.optimization_barrier((lines, held[2], held[4], held[8]))
    lines = exchange(lines, "grid").reshape(parts * share, length)
    both = partner(jnp.stack([held[4], held[8]]), 2)
    held[6], held[10] = both[0], both[1]
    held[12] = partner(held[8], 4)
    held[14] = partner(spectrum, 14)
    away = {}
    for masks in ((0, 2, 4, 8), (6, 10, 12, 14)):
        group = partner(jnp.stack([held[mask] for mask in masks]), 1)
        for i, mask in enumerate(masks):
            away[mask] = group[i]
    near = jnp.stack([held[mask] for mask in range(0, parts, 2)])
    far = jnp.stack([away[mask] for mask in range(0, parts, 2)])
    potential = call(spread_kernel, (parts, 2 * points, length))(lines)
    potential = exchange(potential, "band").reshape(parts, 2, share, share, length)
    base = call(
        base_kernel,
        (2, share, length, length),
        grid=steps,
        in_specs=[
            scalar, scalar, half_block, half_block, orbital_block, trial_block,
            local_block, local_block, table_block, table_block,
        ],
        out_specs=base_block,
    )(
        me.reshape(1),
        band_energies,
        near.reshape(parts // 2, 2, share, share, length),
        far.reshape(parts // 2, 2, share, share, length),
        orbitals,
        trials,
        alda_kernel,
        local_potential,
        tables["up"],
        tables["down"],
    )
    fields = call(
        field_kernel,
        (parts, 2, 2, share, share, length),
        grid=steps,
        in_specs=[share_block, orbital_block, base_block, table_block, table_block],
        out_specs=pl.BlockSpec(
            (parts, 2, 2, ROWS, share, length), lambda i: (0, 0, 0, i, 0, 0)
        ),
    )(potential, orbitals, base, tables["up"], tables["down"])
    received = exchange(fields.reshape(parts, 4 * points, length), "grid")
    shape = (2, 1, share, length, length)
    return tuple(call(final_kernel, [shape, shape])(received, tables["last"]))


def solution(mesh):
    placed = (
        P("band", "grid", None, None),
        P(None, "band", "grid", None, None),
        P("grid", None, None),
        P("grid", None, None),
        P("band"),
    )

    return jax.shard_map(
        per_device,
        mesh=mesh,
        in_specs=placed,
        out_specs=(P(None, "band", "grid", None, None), P(None, "band", "grid", None, None)),
        check_vma=False,
    )
```

```python
import functools
import math

import jax
import jax.numpy as jnp
import numpy as np
from jax import lax
from jax.experimental import pallas as pl
from jax.experimental.pallas import tpu as pltpu
from jax.sharding import PartitionSpec as P


box_length = 30.0
NARROW = jnp.bfloat16
WIDE = jnp.float32
ROWS = 8
GRANT = 20 * 2**20
WIDE_GRANT = 60 * 2**20


def halves(table):
    high = table.astype(np.float32).astype(jnp.bfloat16)
    low = (table - high.astype(np.float64)).astype(np.float32).astype(jnp.bfloat16)
    return np.stack([high, low])


@functools.cache
def make_tables(length):
    wrapped = np.outer(np.arange(length), np.arange(length)) % length
    angles = wrapped.astype(np.float64) * (2.0 * math.pi / length)
    cosine, sine = np.cos(angles), np.sin(angles)
    return {
        "down": halves(np.block([[cosine, sine], [-sine, cosine]])),
        "up": halves(np.block([[cosine, -sine], [sine, cosine]])),
        "last": halves(np.block([[cosine, -sine], [sine, cosine]]) * float(length) ** -1.5),
    }


def split(value):
    high = value.astype(NARROW)
    return high, (value - high.astype(WIDE)).astype(NARROW)


def mul(left, right):
    return lax.dot_general(left, right, (((1,), (0,)), ((), ())), preferred_element_type=WIDE)


def product(left, right):
    left_high, left_low = left
    right_high, right_low = right
    return mul(left_high, right_high) + mul(left_low, right_high) + mul(left_high, right_low)


def pair(ref):
    return ref[0], ref[1]


def swap_blocks(value):
    rows, columns = value.shape[0] // 2, value.shape[1] // 2
    left = jnp.concatenate([value[:rows, :columns], value[rows:, :columns]], axis=1)
    right = jnp.concatenate([value[:rows, columns:], value[rows:, columns:]], axis=1)
    return jnp.concatenate([left, right], axis=0)


def parts_down(value):
    half = value.shape[1] // 2
    return jnp.concatenate([value[:, :half], value[:, half:]], axis=0)


def parts_across(value):
    half = value.shape[0] // 2
    return jnp.concatenate([value[:half], value[half:]], axis=1)


def density_kernel(me_ref, orbital_in, trial_in, up_in, down_in, *refs):
    (
        kept_hbm, near_hbm, out_hbm, orbital_ref, trial_ref, up_ref, down_ref, mixed_ref, out_ref,
        table_sems, row_sems, out_sems,
    ) = refs
    me = me_ref[0]
    length = orbital_ref.shape[2]
    parts, share = out_ref.shape[0], out_ref.shape[3]
    half = orbital_ref.shape[1] // 2
    tables = [
        pltpu.make_async_copy(up_in, up_ref, table_sems.at[0]),
        pltpu.make_async_copy(down_in, down_ref, table_sems.at[1]),
    ]
    rows = [pl.ds(i * half, half) for i in range(2)]
    orbitals, trials = [], []
    for i in range(2):
        part = (slice(None), rows[i])
        orbitals.append(
            pltpu.make_async_copy(orbital_in.at[part], orbital_ref.at[part], row_sems.at[i, 0])
        )
        part = (slice(None), slice(None), rows[i])
        trials.append(
            pltpu.make_async_copy(trial_in.at[part], trial_ref.at[part], row_sems.at[i, 1])
        )
    outs = [
        [
            pltpu.make_async_copy(mixed_ref.at[1], near_hbm, out_sems.at[1]),
            pltpu.make_async_copy(mixed_ref.at[0], kept_hbm, out_sems.at[0]),
        ],
        [pltpu.make_async_copy(out_ref, out_hbm, out_sems.at[2])],
    ]
    for copy in (tables[0], orbitals[0], trials[0], tables[1], orbitals[1], trials[1]):
        copy.start()
    for copy in tables:
        copy.wait()
    for i in range(2):
        orbitals[i].wait()
        trials[i].wait()
        values = []
        for x in range(half):
            orbital = 2.0 * orbital_ref[0, i * half + x].astype(WIDE)
            values.append(
                jnp.concatenate(
                    [trial_ref[k, 0, i * half + x].astype(WIDE) * orbital for k in range(2)], axis=1
                )
            )
        turned = product(split(jnp.concatenate(values, axis=0)), pair(up_ref))
        columns = [parts_down(turned[x * length : (x + 1) * length]) for x in range(half)]
        turned = product(pair(down_ref), split(jnp.concatenate(columns, axis=1)))
        for x in range(half):
            for part in range(2):
                block = turned[part * length : (part + 1) * length, x * length : (x + 1) * length]
                if i == 1:
                    out_ref[:, part, x] = block.reshape(parts, share, length)
                    continue
                for n in range(parts):
                    tile = block[n * share : (n + 1) * share]
                    steps = ((n >> 1) - (me >> 1)) & (parts // 2 - 1)
                    mixed_ref[(n ^ me) & 1, steps, part, x] = tile
        for copy in outs[i]:
            copy.start()
    for copy in outs[0] + outs[1]:
        copy.wait()


def share_kernel(pieces_ref, *refs):
    *near_refs, share_ref, out_ref = refs
    first = near_refs[0][...]
    for ref in near_refs[1:]:
        first = first + ref[...]
    second = pieces_ref[0]
    for i in range(1, pieces_ref.shape[0]):
        second = second + pieces_ref[i]
    rows = first.shape[0] // 2
    for part in range(2):
        held = slice(part * rows, (part + 1) * rows)
        share_ref[2 * part * rows : (2 * part + 1) * rows, :] = first[held]
        share_ref[(2 * part + 1) * rows : 2 * (part + 1) * rows, :] = second[held]
    copies, rows, _ = out_ref.shape
    share = rows // 2
    for b in range(share):
        block = share_ref[pl.ds(b, rows, stride=share), :]
        for i in range(copies // share):
            out_ref[b * (copies // share) + i] = block


def line_kernel(pieces_ref, kernel_ref, down_ref, up_ref, out_ref):
    parts, rows, length = pieces_ref.shape
    share = rows // 2
    columns = jnp.concatenate(
        [pieces_ref[:, :share, :].reshape(length, length), pieces_ref[:, share:, :].reshape(length, length)],
        axis=0,
    )
    turned = product(pair(down_ref), split(columns))
    kernel = kernel_ref[...]
    turned = turned * jnp.concatenate([kernel, kernel], axis=0)
    out_ref[...] = product(pair(up_ref), split(turned)).reshape(parts, share, length)


def spread_kernel(pieces_ref, out_ref):
    share = pieces_ref.shape[0] // out_ref.shape[0]
    for part in range(2):
        for x in range(share):
            block = pieces_ref[pl.ds(part * share + x, share, stride=2 * share), :]
            rows = pl.ds((part * share + x) * share, share)
            for i in range(out_ref.shape[0]):
                out_ref[i, rows, :] = block


def back(blocks, up_ref, down_ref, length):
    turned = product(pair(up_ref), split(blocks))
    rows = turned.shape[1] // length
    points = [parts_across(turned[:, x * length : (x + 1) * length]) for x in range(rows)]
    return product(split(jnp.concatenate(points, axis=0)), pair(down_ref))


def base_kernel(
    me_ref, energy_ref, near_ref, far_ref, orbital_ref, trial_ref, alda_ref, local_ref,
    up_ref, down_ref, out_ref,
):
    length = orbital_ref.shape[2]
    parts = 2 * near_ref.shape[0]
    me = me_ref[0]
    energy = energy_ref[0]
    even = (me & 1) == 0
    scale = 1.0 / float(length * length)
    rows = orbital_ref.shape[1]
    columns = []
    for x in range(rows):
        tiles = []
        for part in range(2):
            for half in range(parts // 2):
                slot = half ^ (me >> 1)
                near = near_ref[slot, part, x]
                far = far_ref[slot, part, x]
                tiles.append(jnp.where(even, near, far))
                tiles.append(jnp.where(even, far, near))
        columns.append(jnp.concatenate(tiles, axis=0))
    value = back(jnp.concatenate(columns, axis=1), up_ref, down_ref, length)
    for x in range(rows):
        factor = orbital_ref[0, x].astype(WIDE) * (alda_ref[x] * scale)
        weight = local_ref[x] - energy
        for k in range(2):
            block = value[x * length : (x + 1) * length, k * length : (k + 1) * length]
            out_ref[k, x] = block * factor + weight * trial_ref[k, 0, x].astype(WIDE)


def field_kernel(potential_ref, orbital_ref, base_ref, up_ref, down_ref, out_ref):
    length = orbital_ref.shape[2]
    parts = potential_ref.shape[0]
    rows = orbital_ref.shape[1]
    columns = []
    for x in range(rows):
        columns.append(
            jnp.concatenate(
                [potential_ref[:, part, x].reshape(length, length) for part in range(2)], axis=0
            )
        )
    value = back(jnp.concatenate(columns, axis=1), up_ref, down_ref, length)
    fields = []
    for x in range(rows):
        orbital = orbital_ref[0, x].astype(WIDE)
        for k in range(2):
            block = value[x * length : (x + 1) * length, k * length : (k + 1) * length]
            fields.append(block * orbital + base_ref[k, x])
    table = (up_ref[0, :length, :], up_ref[1, :length, :])
    turned = product(split(jnp.concatenate(fields, axis=0)), table)
    for x in range(rows):
        points = swap_blocks(turned[2 * x * length : 2 * (x + 1) * length])
        waves = product(pair(down_ref), split(points))
        for k in range(2):
            for part in range(2):
                block = waves[part * length : (part + 1) * length, k * length : (k + 1) * length]
                out_ref[:, k, part, x] = block.reshape(parts, length // parts, length)


def final_kernel(pieces_ref, x_ref, real_ref, imag_ref):
    length = real_ref.shape[-1]
    share = real_ref.shape[2]
    table = pair(x_ref)
    for k in range(2):
        for b in range(share):
            parts = []
            for part in range(2):
                start = (k * 2 + part) * share * share + b
                block = pieces_ref[:, pl.ds(start, share, stride=share), :]
                parts.append(block.reshape(length, length))
            turned = product(split(jnp.concatenate(parts, axis=0).T), table)
            real_ref[k, 0, b] = turned[:, :length]
            imag_ref[k, 0, b] = turned[:, length:]


def signed(positions, length):
    return jnp.where(2 * positions < length, positions, positions - length).astype(WIDE)


def line_coulomb(b, length):
    a = lax.broadcasted_iota(jnp.int32, (length, length), 0)
    c = lax.broadcasted_iota(jnp.int32, (length, length), 1)
    squared = signed(a, length) ** 2 + signed(b, length) ** 2 + signed(c, length) ** 2
    scaled = box_length**2 / math.pi / jnp.maximum(squared, 1.0)
    return jnp.where(squared > 0, scaled, 0.0) / float(length**3)


def call(body, shapes, grant=GRANT, **options):
    return pl.pallas_call(
        body,
        out_shape=jax.tree.map(
            lambda s: jax.ShapeDtypeStruct(s, WIDE),
            shapes,
            is_leaf=lambda s: isinstance(s, tuple) and isinstance(s[0], int),
        ),
        compiler_params=pltpu.CompilerParams(vmem_limit_bytes=grant),
        **options,
    )


def exchange(array, axis):
    return lax.all_to_all(array, axis, split_axis=0, concat_axis=0, tiled=True)


def partner(array, mask):
    return lax.ppermute(array, "band", [(i, i ^ mask) for i in range(lax.axis_size("band"))])


def ahead(array, steps):
    count = lax.axis_size("band")
    return lax.ppermute(array, "band", [(i, (i + steps) % count) for i in range(count)])


def per_device(orbitals, trials, alda_kernel, local_potential, band_energies):
    length = orbitals.shape[2]
    parts = lax.axis_size("band")
    share = length // parts
    points = share * share
    tables = {name: jnp.asarray(table) for name, table in make_tables(length).items()}
    me = lax.axis_index("band")
    place = lax.axis_index("grid")
    copies = parts // share
    kernel = line_coulomb(me * share + place // copies, length)
    own_up = lax.dynamic_slice_in_dim(tables["up"], (place % copies) * length, length, 1)

    scalar = pl.BlockSpec(memory_space=pltpu.SMEM)
    orbital_block = pl.BlockSpec((1, ROWS, length, length), lambda i: (0, i, 0, 0))
    trial_block = pl.BlockSpec((2, 1, ROWS, length, length), lambda i: (0, 0, i, 0, 0))
    table_block = pl.BlockSpec((2, 2 * length, 2 * length), lambda i: (0, 0, 0))
    share_block = pl.BlockSpec((parts, 2, ROWS, share, length), lambda i: (0, 0, i, 0, 0))
    half_block = pl.BlockSpec((parts // 2, 2, ROWS, share, length), lambda i: (0, 0, i, 0, 0))
    local_block = pl.BlockSpec((ROWS, length, length), lambda i: (i, 0, 0))
    base_block = pl.BlockSpec((2, ROWS, length, length), lambda i: (0, i, 0, 0))
    steps = (share // ROWS,)

    held = pl.BlockSpec(memory_space=pltpu.HBM)
    half = share // 2
    some = (parts // 2, 2, half, share, length)
    kept, near, pieces = call(
        density_kernel,
        [some, some, (parts, 2, half, share, length)],
        grant=WIDE_GRANT,
        in_specs=[scalar] + [held] * 4,
        out_specs=[held] * 3,
        scratch_shapes=[
            pltpu.VMEM(orbitals.shape, NARROW),
            pltpu.VMEM(trials.shape, NARROW),
            pltpu.VMEM(tables["up"].shape, NARROW),
            pltpu.VMEM(tables["down"].shape, NARROW),
            pltpu.VMEM((2, *some), WIDE),
            pltpu.VMEM((parts, 2, half, share, length), WIDE),
            pltpu.SemaphoreType.DMA((2,)),
            pltpu.SemaphoreType.DMA((2, 2)),
            pltpu.SemaphoreType.DMA((3,)),
        ],
    )(me.reshape(1), orbitals, trials, tables["up"], tables["down"])
    near = partner(near.reshape(parts // 2, points, length), 1)
    near = near + kept.reshape(parts // 2, points, length)
    near = [near[0]] + [ahead(near[i], 2 * i) for i in range(1, parts // 2)]
    pieces = exchange(pieces.reshape(parts, points, length), "band")
    spectrum, lines = call(
        share_kernel, [(2 * points, length), (parts, 2 * share, length)]
    )(pieces, *near)
    lines = exchange(lines, "grid")
    held = {0: spectrum}
    for mask in (2, 4, 8):
        held[mask] = partner(spectrum, mask)
    lines = call(line_kernel, (parts, share, length))(
        lines, kernel, tables["down"], own_up
    )
    _, held[2], held[4], held[8] = lax.optimization_barrier((lines, held[2], held[4], held[8]))
    lines = exchange(lines, "grid").reshape(parts * share, length)
    both = partner(jnp.stack([held[4], held[8]]), 2)
    held[6], held[10] = both[0], both[1]
    held[12] = partner(held[8], 4)
    held[14] = partner(spectrum, 14)
    away = {}
    for masks in ((0, 2, 4, 8), (6, 10, 12, 14)):
        group = partner(jnp.stack([held[mask] for mask in masks]), 1)
        for i, mask in enumerate(masks):
            away[mask] = group[i]
    near = jnp.stack([held[mask] for mask in range(0, parts, 2)])
    far = jnp.stack([away[mask] for mask in range(0, parts, 2)])
    potential = call(spread_kernel, (parts, 2 * points, length))(lines)
    potential = exchange(potential, "band").reshape(parts, 2, share, share, length)
    base = call(
        base_kernel,
        (2, share, length, length),
        grid=steps,
        in_specs=[
            scalar, scalar, half_block, half_block, orbital_block, trial_block,
            local_block, local_block, table_block, table_block,
        ],
        out_specs=base_block,
    )(
        me.reshape(1),
        band_energies,
        near.reshape(parts // 2, 2, share, share, length),
        far.reshape(parts // 2, 2, share, share, length),
        orbitals,
        trials,
        alda_kernel,
        local_potential,
        tables["up"],
        tables["down"],
    )
    fields = call(
        field_kernel,
        (parts, 2, 2, share, share, length),
        grid=steps,
        in_specs=[share_block, orbital_block, base_block, table_block, table_block],
        out_specs=pl.BlockSpec(
            (parts, 2, 2, ROWS, share, length), lambda i: (0, 0, 0, i, 0, 0)
        ),
    )(potential, orbitals, base, tables["up"], tables["down"])
    received = exchange(fields.reshape(parts, 4 * points, length), "grid")
    shape = (2, 1, share, length, length)
    return tuple(call(final_kernel, [shape, shape])(received, tables["last"]))


def solution(mesh):
    placed = (
        P("band", "grid", None, None),
        P(None, "band", "grid", None, None),
        P("grid", None, None),
        P("grid", None, None),
        P("band"),
    )

    return jax.shard_map(
        per_device,
        mesh=mesh,
        in_specs=placed,
        out_specs=(P(None, "band", "grid", None, None), P(None, "band", "grid", None, None)),
        check_vma=False,
    )
```

```python
import functools
import math

import jax
import jax.numpy as jnp
import numpy as np
from jax import lax
from jax.experimental import pallas as pl
from jax.experimental.pallas import tpu as pltpu
from jax.sharding import PartitionSpec as P


box_length = 30.0
NARROW = jnp.bfloat16
WIDE = jnp.float32
ROWS = 8
GRANT = 20 * 2**20
WIDE_GRANT = 60 * 2**20


def halves(table):
    high = table.astype(np.float32).astype(jnp.bfloat16)
    low = (table - high.astype(np.float64)).astype(np.float32).astype(jnp.bfloat16)
    return np.stack([high, low])


@functools.cache
def make_tables(length):
    wrapped = np.outer(np.arange(length), np.arange(length)) % length
    angles = wrapped.astype(np.float64) * (2.0 * math.pi / length)
    cosine, sine = np.cos(angles), np.sin(angles)
    return {
        "down": halves(np.block([[cosine, sine], [-sine, cosine]])),
        "up": halves(np.block([[cosine, -sine], [sine, cosine]])),
        "last": halves(np.block([[cosine, -sine], [sine, cosine]]) * float(length) ** -1.5),
    }


def split(value):
    high = value.astype(NARROW)
    return high, (value - high.astype(WIDE)).astype(NARROW)


def mul(left, right):
    return lax.dot_general(left, right, (((1,), (0,)), ((), ())), preferred_element_type=WIDE)


def product(left, right):
    left_high, left_low = left
    right_high, right_low = right
    return mul(left_high, right_high) + mul(left_low, right_high) + mul(left_high, right_low)


def pair(ref):
    return ref[0], ref[1]


def swap_blocks(value):
    rows, columns = value.shape[0] // 2, value.shape[1] // 2
    left = jnp.concatenate([value[:rows, :columns], value[rows:, :columns]], axis=1)
    right = jnp.concatenate([value[:rows, columns:], value[rows:, columns:]], axis=1)
    return jnp.concatenate([left, right], axis=0)


def parts_down(value):
    half = value.shape[1] // 2
    return jnp.concatenate([value[:, :half], value[:, half:]], axis=0)


def parts_across(value):
    half = value.shape[0] // 2
    return jnp.concatenate([value[:half], value[half:]], axis=1)


def density_kernel(me_ref, orbital_in, trial_in, up_in, down_in, *refs):
    (
        kept_hbm, near_hbm, out_hbm, orbital_ref, trial_ref, up_ref, down_ref, mixed_ref, out_ref,
        table_sems, row_sems, out_sems,
    ) = refs
    me = me_ref[0]
    length = orbital_ref.shape[2]
    parts, share = out_ref.shape[0], out_ref.shape[3]
    half = orbital_ref.shape[1] // 2
    tables = [
        pltpu.make_async_copy(up_in, up_ref, table_sems.at[0]),
        pltpu.make_async_copy(down_in, down_ref, table_sems.at[1]),
    ]
    rows = [pl.ds(i * half, half) for i in range(2)]
    orbitals, trials = [], []
    for i in range(2):
        part = (slice(None), rows[i])
        orbitals.append(
            pltpu.make_async_copy(orbital_in.at[part], orbital_ref.at[part], row_sems.at[i, 0])
        )
        part = (slice(None), slice(None), rows[i])
        trials.append(
            pltpu.make_async_copy(trial_in.at[part], trial_ref.at[part], row_sems.at[i, 1])
        )
    outs = [
        [
            pltpu.make_async_copy(mixed_ref.at[1], near_hbm, out_sems.at[1]),
            pltpu.make_async_copy(mixed_ref.at[0], kept_hbm, out_sems.at[0]),
        ],
        [pltpu.make_async_copy(out_ref, out_hbm, out_sems.at[2])],
    ]
    for copy in (tables[0], orbitals[0], trials[0], tables[1], orbitals[1], trials[1]):
        copy.start()
    for copy in tables:
        copy.wait()
    for i in range(2):
        orbitals[i].wait()
        trials[i].wait()
        values = []
        for x in range(half):
            orbital = 2.0 * orbital_ref[0, i * half + x].astype(WIDE)
            values.append(
                jnp.concatenate(
                    [trial_ref[k, 0, i * half + x].astype(WIDE) * orbital for k in range(2)], axis=1
                )
            )
        turned = product(split(jnp.concatenate(values, axis=0)), pair(up_ref))
        columns = [parts_down(turned[x * length : (x + 1) * length]) for x in range(half)]
        turned = product(pair(down_ref), split(jnp.concatenate(columns, axis=1)))
        for x in range(half):
            for part in range(2):
                block = turned[part * length : (part + 1) * length, x * length : (x + 1) * length]
                if i == 1:
                    out_ref[:, part, x] = block.reshape(parts, share, length)
                    continue
                for n in range(parts):
                    tile = block[n * share : (n + 1) * share]
                    mixed_ref[(n ^ me) & 1, (n ^ me) >> 1, part, x] = tile
        for copy in outs[i]:
            copy.start()
    for copy in outs[0] + outs[1]:
        copy.wait()


def share_kernel(pieces_ref, *refs):
    *near_refs, share_ref, out_ref = refs
    first = near_refs[0][...]
    for ref in near_refs[1:]:
        first = first + ref[...]
    second = pieces_ref[0]
    for i in range(1, pieces_ref.shape[0]):
        second = second + pieces_ref[i]
    rows = first.shape[0] // 2
    for part in range(2):
        held = slice(part * rows, (part + 1) * rows)
        share_ref[2 * part * rows : (2 * part + 1) * rows, :] = first[held]
        share_ref[(2 * part + 1) * rows : 2 * (part + 1) * rows, :] = second[held]
    copies, rows, _ = out_ref.shape
    share = rows // 2
    for b in range(share):
        block = share_ref[pl.ds(b, rows, stride=share), :]
        for i in range(copies // share):
            out_ref[b * (copies // share) + i] = block


def line_kernel(pieces_ref, kernel_ref, down_ref, up_ref, out_ref):
    parts, rows, length = pieces_ref.shape
    share = rows // 2
    columns = jnp.concatenate(
        [pieces_ref[:, :share, :].reshape(length, length), pieces_ref[:, share:, :].reshape(length, length)],
        axis=0,
    )
    turned = product(pair(down_ref), split(columns))
    kernel = kernel_ref[...]
    turned = turned * jnp.concatenate([kernel, kernel], axis=0)
    out_ref[...] = product(pair(up_ref), split(turned)).reshape(parts, share, length)


def spread_kernel(pieces_ref, out_ref, own_ref):
    parts, _, _ = out_ref.shape
    share = pieces_ref.shape[0] // parts
    half = share // 2
    for part in range(2):
        for x in range(share):
            block = pieces_ref[pl.ds(part * share + x, share, stride=2 * share), :]
            rows = pl.ds((part * half + x % half) * share, share)
            if x >= half:
                own_ref[rows, :] = block
                continue
            for i in range(parts):
                out_ref[i, rows, :] = block


def all_columns(me, near_ref, far_ref, x):
    even = (me & 1) == 0
    tiles = []
    for part in range(2):
        for half in range(near_ref.shape[0]):
            slot = half ^ (me >> 1)
            near = near_ref[slot, part, x]
            far = far_ref[slot, part, x]
            tiles.append(jnp.where(even, near, far))
            tiles.append(jnp.where(even, far, near))
    return jnp.concatenate(tiles, axis=0)


def back(blocks, up_ref, down_ref, length):
    turned = product(pair(up_ref), split(blocks))
    rows = turned.shape[1] // length
    points = [parts_across(turned[:, x * length : (x + 1) * length]) for x in range(rows)]
    return product(split(jnp.concatenate(points, axis=0)), pair(down_ref))


def base_kernel(
    me_ref, energy_ref, near_ref, far_ref, orbital_ref, trial_ref, alda_ref, local_ref,
    up_ref, down_ref, out_ref,
):
    length = orbital_ref.shape[2]
    me = me_ref[0]
    energy = energy_ref[0]
    scale = 1.0 / float(length * length)
    rows = orbital_ref.shape[1]
    columns = [all_columns(me, near_ref, far_ref, x) for x in range(rows)]
    value = back(jnp.concatenate(columns, axis=1), up_ref, down_ref, length)
    for x in range(rows):
        factor = orbital_ref[0, x].astype(WIDE) * (alda_ref[x] * scale)
        weight = local_ref[x] - energy
        for k in range(2):
            block = value[x * length : (x + 1) * length, k * length : (k + 1) * length]
            out_ref[k, x] = block * factor + weight * trial_ref[k, 0, x].astype(WIDE)


def field_kernel(me_ref, potential_ref, *refs):
    *share_refs, orbital_ref, base_ref, up_ref, down_ref, out_ref, near_ref, far_ref = refs
    length = orbital_ref.shape[2]
    parts = potential_ref.shape[0]
    rows = orbital_ref.shape[1]
    count = near_ref.shape[0]
    for i in range(count):
        near_ref[i] = share_refs[i][...]
    start = 0
    for ref in share_refs[count:]:
        far_ref[start : start + ref.shape[0]] = ref[...]
        start += ref.shape[0]
    columns = []
    for x in range(rows // 2):
        columns.append(
            jnp.concatenate(
                [potential_ref[:, part, x].reshape(length, length) for part in range(2)], axis=0
            )
        )
    columns += [all_columns(me_ref[0], near_ref, far_ref, x) for x in range(rows // 2)]
    value = back(jnp.concatenate(columns, axis=1), up_ref, down_ref, length)
    fields = []
    for x in range(rows):
        orbital = orbital_ref[0, x].astype(WIDE)
        for k in range(2):
            block = value[x * length : (x + 1) * length, k * length : (k + 1) * length]
            fields.append(block * orbital + base_ref[k, x])
    table = (up_ref[0, :length, :], up_ref[1, :length, :])
    turned = product(split(jnp.concatenate(fields, axis=0)), table)
    for x in range(rows):
        points = swap_blocks(turned[2 * x * length : 2 * (x + 1) * length])
        waves = product(pair(down_ref), split(points))
        for k in range(2):
            for part in range(2):
                block = waves[part * length : (part + 1) * length, k * length : (k + 1) * length]
                out_ref[:, k, part, x] = block.reshape(parts, length // parts, length)


def final_kernel(pieces_ref, x_ref, real_ref, imag_ref):
    length = real_ref.shape[-1]
    share = real_ref.shape[2]
    table = pair(x_ref)
    for k in range(2):
        for b in range(share):
            parts = []
            for part in range(2):
                start = (k * 2 + part) * share * share + b
                block = pieces_ref[:, pl.ds(start, share, stride=share), :]
                parts.append(block.reshape(length, length))
            turned = product(split(jnp.concatenate(parts, axis=0).T), table)
            real_ref[k, 0, b] = turned[:, :length]
            imag_ref[k, 0, b] = turned[:, length:]


def signed(positions, length):
    return jnp.where(2 * positions < length, positions, positions - length).astype(WIDE)


def line_coulomb(b, length):
    a = lax.broadcasted_iota(jnp.int32, (length, length), 0)
    c = lax.broadcasted_iota(jnp.int32, (length, length), 1)
    squared = signed(a, length) ** 2 + signed(b, length) ** 2 + signed(c, length) ** 2
    scaled = box_length**2 / math.pi / jnp.maximum(squared, 1.0)
    return jnp.where(squared > 0, scaled, 0.0) / float(length**3)


def call(body, shapes, grant=GRANT, **options):
    return pl.pallas_call(
        body,
        out_shape=jax.tree.map(
            lambda s: jax.ShapeDtypeStruct(s, WIDE),
            shapes,
            is_leaf=lambda s: isinstance(s, tuple) and isinstance(s[0], int),
        ),
        compiler_params=pltpu.CompilerParams(vmem_limit_bytes=grant),
        **options,
    )


def exchange(array, axis):
    return lax.all_to_all(array, axis, split_axis=0, concat_axis=0, tiled=True)


def partner(array, mask):
    return lax.ppermute(array, "band", [(i, i ^ mask) for i in range(lax.axis_size("band"))])


def per_device(orbitals, trials, alda_kernel, local_potential, band_energies):
    length = orbitals.shape[2]
    parts = lax.axis_size("band")
    share = length // parts
    points = share * share
    tables = {name: jnp.asarray(table) for name, table in make_tables(length).items()}
    me = lax.axis_index("band")
    place = lax.axis_index("grid")
    copies = parts // share
    kernel = line_coulomb(me * share + place // copies, length)
    own_up = lax.dynamic_slice_in_dim(tables["up"], (place % copies) * length, length, 1)

    scalar = pl.BlockSpec(memory_space=pltpu.SMEM)
    orbital_block = pl.BlockSpec((1, ROWS, length, length), lambda i: (0, i, 0, 0))
    trial_block = pl.BlockSpec((2, 1, ROWS, length, length), lambda i: (0, 0, i, 0, 0))
    table_block = pl.BlockSpec((2, 2 * length, 2 * length), lambda i: (0, 0, 0))
    half_block = pl.BlockSpec((parts // 2, 2, ROWS, share, length), lambda i: (0, 0, i, 0, 0))
    local_block = pl.BlockSpec((ROWS, length, length), lambda i: (i, 0, 0))
    base_block = pl.BlockSpec((2, ROWS, length, length), lambda i: (0, i, 0, 0))
    steps = (share // ROWS,)

    held = pl.BlockSpec(memory_space=pltpu.HBM)
    half = share // 2
    some = (parts // 2, 2, half, share, length)
    kept, near, pieces = call(
        density_kernel,
        [some, some, (parts, 2, half, share, length)],
        grant=WIDE_GRANT,
        in_specs=[scalar] + [held] * 4,
        out_specs=[held] * 3,
        scratch_shapes=[
            pltpu.VMEM(orbitals.shape, NARROW),
            pltpu.VMEM(trials.shape, NARROW),
            pltpu.VMEM(tables["up"].shape, NARROW),
            pltpu.VMEM(tables["down"].shape, NARROW),
            pltpu.VMEM((2, *some), WIDE),
            pltpu.VMEM((parts, 2, half, share, length), WIDE),
            pltpu.SemaphoreType.DMA((2,)),
            pltpu.SemaphoreType.DMA((2, 2)),
            pltpu.SemaphoreType.DMA((3,)),
        ],
    )(me.reshape(1), orbitals, trials, tables["up"], tables["down"])
    near = partner(near.reshape(parts // 2, points, length), 1)
    near = near + kept.reshape(parts // 2, points, length)
    near = [near[0]] + [partner(near[i], 2 * i) for i in range(1, parts // 2)]
    pieces = exchange(pieces.reshape(parts, points, length), "band")
    spectrum, lines = call(
        share_kernel, [(2 * points, length), (parts, 2 * share, length)]
    )(pieces, *near)
    lines = exchange(lines, "grid")
    held = {0: spectrum}
    for mask in (2, 4, 8):
        held[mask] = partner(spectrum, mask)
    lines = call(line_kernel, (parts, share, length))(
        lines, kernel, tables["down"], own_up
    )
    _, held[2], held[4], held[8] = lax.optimization_barrier((lines, held[2], held[4], held[8]))
    lines = exchange(lines, "grid").reshape(parts * share, length)
    both = partner(jnp.stack([held[4], held[8]]), 2)
    held[6], held[10] = both[0], both[1]
    held[12] = partner(held[8], 4)
    held[14] = partner(spectrum, 14)
    away = {}
    for masks in ((0, 2, 4, 8), (6, 10, 12, 14)):
        group = partner(jnp.stack([held[mask] for mask in masks]), 1)
        for i, mask in enumerate(masks):
            away[mask] = group[i]
    near = jnp.stack([held[mask] for mask in range(0, parts, 2)])
    far = jnp.stack([away[mask] for mask in range(0, parts, 2)])
    potential, own = call(spread_kernel, [(parts, points, length), (points, length)])(lines)
    potential = exchange(potential, "band").reshape(
        parts, 2, half, share, length
    )
    gained = {0: own}
    for masks in ((2, 4, 6), (8, 10, 12, 14)):
        for mask in masks:
            gained[mask] = partner(own, mask)
    passed = [
        partner(jnp.stack([gained[mask] for mask in masks]), 1)
        for masks in ((0, 2, 4, 6), (8, 10, 12, 14))
    ]
    spread = [gained[mask].reshape(2, half, share, length) for mask in range(0, parts, 2)]
    spread += [array.reshape(-1, 2, half, share, length) for array in passed]
    base = call(
        base_kernel,
        (2, share, length, length),
        grid=steps,
        in_specs=[
            scalar, scalar, half_block, half_block, orbital_block, trial_block,
            local_block, local_block, table_block, table_block,
        ],
        out_specs=base_block,
    )(
        me.reshape(1),
        band_energies,
        near.reshape(parts // 2, 2, share, share, length),
        far.reshape(parts // 2, 2, share, share, length),
        orbitals,
        trials,
        alda_kernel,
        local_potential,
        tables["up"],
        tables["down"],
    )
    vector = pl.BlockSpec(memory_space=pltpu.VMEM)
    shares = pltpu.VMEM(some, WIDE)
    fields = call(
        field_kernel,
        (parts, 2, 2, share, share, length),
        in_specs=[scalar] + [vector] * (len(spread) + 5),
        scratch_shapes=[shares, shares],
    )(me.reshape(1), potential, *spread, orbitals, base, tables["up"], tables["down"])
    received = exchange(fields.reshape(parts, 4 * points, length), "grid")
    shape = (2, 1, share, length, length)
    return tuple(call(final_kernel, [shape, shape])(received, tables["last"]))


def solution(mesh):
    placed = (
        P("band", "grid", None, None),
        P(None, "band", "grid", None, None),
        P("grid", None, None),
        P("grid", None, None),
        P("band"),
    )

    return jax.shard_map(
        per_device,
        mesh=mesh,
        in_specs=placed,
        out_specs=(P(None, "band", "grid", None, None), P(None, "band", "grid", None, None)),
        check_vma=False,
    )
```

```python
import functools
import math

import jax
import jax.numpy as jnp
import numpy as np
from jax import lax
from jax.experimental import pallas as pl
from jax.experimental.pallas import tpu as pltpu
from jax.sharding import PartitionSpec as P


box_length = 30.0
NARROW = jnp.bfloat16
WIDE = jnp.float32
ROWS = 8
GRANT = 20 * 2**20
WIDE_GRANT = 60 * 2**20


def halves(table):
    high = table.astype(np.float32).astype(jnp.bfloat16)
    low = (table - high.astype(np.float64)).astype(np.float32).astype(jnp.bfloat16)
    return np.stack([high, low])


@functools.cache
def make_tables(length):
    wrapped = np.outer(np.arange(length), np.arange(length)) % length
    angles = wrapped.astype(np.float64) * (2.0 * math.pi / length)
    cosine, sine = np.cos(angles), np.sin(angles)
    return {
        "down": halves(np.block([[cosine, sine], [-sine, cosine]])),
        "up": halves(np.block([[cosine, -sine], [sine, cosine]])),
        "last": halves(np.block([[cosine, -sine], [sine, cosine]]) * float(length) ** -1.5),
    }


def split(value):
    high = value.astype(NARROW)
    return high, (value - high.astype(WIDE)).astype(NARROW)


def mul(left, right):
    return lax.dot_general(left, right, (((1,), (0,)), ((), ())), preferred_element_type=WIDE)


def product(left, right):
    left_high, left_low = left
    right_high, right_low = right
    return mul(left_high, right_high) + mul(left_low, right_high) + mul(left_high, right_low)


def pair(ref):
    return ref[0], ref[1]


def swap_blocks(value):
    rows, columns = value.shape[0] // 2, value.shape[1] // 2
    left = jnp.concatenate([value[:rows, :columns], value[rows:, :columns]], axis=1)
    right = jnp.concatenate([value[:rows, columns:], value[rows:, columns:]], axis=1)
    return jnp.concatenate([left, right], axis=0)


def parts_down(value):
    half = value.shape[1] // 2
    return jnp.concatenate([value[:, :half], value[:, half:]], axis=0)


def parts_across(value):
    half = value.shape[0] // 2
    return jnp.concatenate([value[:half], value[half:]], axis=1)


def density_kernel(me_ref, orbital_in, trial_in, up_in, down_in, *refs):
    (
        kept_hbm, near_hbm, out_hbm, orbital_ref, trial_ref, up_ref, down_ref, mixed_ref, out_ref,
        table_sems, row_sems, out_sems,
    ) = refs
    me = me_ref[0]
    length = orbital_ref.shape[2]
    parts, share = out_ref.shape[0], out_ref.shape[3]
    half = orbital_ref.shape[1] // 2
    tables = [
        pltpu.make_async_copy(up_in, up_ref, table_sems.at[0]),
        pltpu.make_async_copy(down_in, down_ref, table_sems.at[1]),
    ]
    rows = [pl.ds(i * half, half) for i in range(2)]
    orbitals, trials = [], []
    for i in range(2):
        part = (slice(None), rows[i])
        orbitals.append(
            pltpu.make_async_copy(orbital_in.at[part], orbital_ref.at[part], row_sems.at[i, 0])
        )
        part = (slice(None), slice(None), rows[i])
        trials.append(
            pltpu.make_async_copy(trial_in.at[part], trial_ref.at[part], row_sems.at[i, 1])
        )
    outs = [
        [
            pltpu.make_async_copy(mixed_ref.at[1], near_hbm, out_sems.at[1]),
            pltpu.make_async_copy(mixed_ref.at[0], kept_hbm, out_sems.at[0]),
        ],
        [pltpu.make_async_copy(out_ref, out_hbm, out_sems.at[2])],
    ]
    for copy in (tables[0], orbitals[0], trials[0], tables[1], orbitals[1], trials[1]):
        copy.start()
    for copy in tables:
        copy.wait()
    for i in range(2):
        orbitals[i].wait()
        trials[i].wait()
        values = []
        for x in range(half):
            orbital = 2.0 * orbital_ref[0, i * half + x].astype(WIDE)
            values.append(
                jnp.concatenate(
                    [trial_ref[k, 0, i * half + x].astype(WIDE) * orbital for k in range(2)], axis=1
                )
            )
        turned = product(split(jnp.concatenate(values, axis=0)), pair(up_ref))
        columns = [parts_down(turned[x * length : (x + 1) * length]) for x in range(half)]
        turned = product(pair(down_ref), split(jnp.concatenate(columns, axis=1)))
        for x in range(half):
            for part in range(2):
                block = turned[part * length : (part + 1) * length, x * length : (x + 1) * length]
                if i == 1:
                    out_ref[:, part, x] = block.reshape(parts, share, length)
                    continue
                for n in range(parts):
                    tile = block[n * share : (n + 1) * share]
                    mixed_ref[(n ^ me) & 1, (n ^ me) >> 1, part, x] = tile
        for copy in outs[i]:
            copy.start()
    for copy in outs[0] + outs[1]:
        copy.wait()


def share_kernel(pieces_ref, *refs):
    *near_refs, share_ref, out_ref = refs
    first = near_refs[0][...]
    for ref in near_refs[1:]:
        first = first + ref[...]
    second = pieces_ref[0]
    for i in range(1, pieces_ref.shape[0]):
        second = second + pieces_ref[i]
    rows = first.shape[0] // 2
    for part in range(2):
        held = slice(part * rows, (part + 1) * rows)
        share_ref[2 * part * rows : (2 * part + 1) * rows, :] = first[held]
        share_ref[(2 * part + 1) * rows : 2 * (part + 1) * rows, :] = second[held]
    copies, rows, _ = out_ref.shape
    share = rows // 2
    for b in range(share):
        block = share_ref[pl.ds(b, rows, stride=share), :]
        for i in range(copies // share):
            out_ref[b * (copies // share) + i] = block


def line_kernel(pieces_ref, kernel_ref, down_ref, up_ref, out_ref):
    parts, rows, length = pieces_ref.shape
    share = rows // 2
    columns = jnp.concatenate(
        [pieces_ref[:, :share, :].reshape(length, length), pieces_ref[:, share:, :].reshape(length, length)],
        axis=0,
    )
    turned = product(pair(down_ref), split(columns))
    kernel = kernel_ref[...]
    turned = turned * jnp.concatenate([kernel, kernel], axis=0)
    out_ref[...] = product(pair(up_ref), split(turned)).reshape(parts, share, length)


def spread_kernel(pieces_ref, out_ref):
    share = pieces_ref.shape[0] // out_ref.shape[0]
    for part in range(2):
        for x in range(share):
            block = pieces_ref[pl.ds(part * share + x, share, stride=2 * share), :]
            rows = pl.ds((part * share + x) * share, share)
            for i in range(out_ref.shape[0]):
                out_ref[i, rows, :] = block


def back(blocks, up_ref, down_ref, length):
    turned = product(pair(up_ref), split(blocks))
    rows = turned.shape[1] // length
    points = [parts_across(turned[:, x * length : (x + 1) * length]) for x in range(rows)]
    return product(split(jnp.concatenate(points, axis=0)), pair(down_ref))


def base_kernel(
    me_ref, energy_ref, near_ref, far_ref, orbital_ref, trial_ref, alda_ref, local_ref,
    up_ref, down_ref, out_ref,
):
    length = orbital_ref.shape[2]
    parts = 2 * near_ref.shape[0]
    me = me_ref[0]
    energy = energy_ref[0]
    even = (me & 1) == 0
    scale = 1.0 / float(length * length)
    rows = orbital_ref.shape[1]
    columns = []
    for x in range(rows):
        tiles = []
        for part in range(2):
            for half in range(parts // 2):
                slot = half ^ (me >> 1)
                near = near_ref[slot, part, x]
                far = far_ref[slot, part, x]
                tiles.append(jnp.where(even, near, far))
                tiles.append(jnp.where(even, far, near))
        columns.append(jnp.concatenate(tiles, axis=0))
    value = back(jnp.concatenate(columns, axis=1), up_ref, down_ref, length)
    for x in range(rows):
        factor = orbital_ref[0, x].astype(WIDE) * (alda_ref[x] * scale)
        weight = local_ref[x] - energy
        for k in range(2):
            block = value[x * length : (x + 1) * length, k * length : (k + 1) * length]
            out_ref[k, x] = block * factor + weight * trial_ref[k, 0, x].astype(WIDE)


def field_kernel(potential_ref, orbital_ref, base_ref, up_ref, down_ref, out_ref):
    length = orbital_ref.shape[2]
    parts = potential_ref.shape[0]
    rows = orbital_ref.shape[1]
    columns = []
    for x in range(rows):
        columns.append(
            jnp.concatenate(
                [potential_ref[:, part, x].reshape(length, length) for part in range(2)], axis=0
            )
        )
    value = back(jnp.concatenate(columns, axis=1), up_ref, down_ref, length)
    fields = []
    for x in range(rows):
        orbital = orbital_ref[0, x].astype(WIDE)
        for k in range(2):
            block = value[x * length : (x + 1) * length, k * length : (k + 1) * length]
            fields.append(block * orbital + base_ref[k, x])
    table = (up_ref[0, :length, :], up_ref[1, :length, :])
    turned = product(split(jnp.concatenate(fields, axis=0)), table)
    for x in range(rows):
        points = swap_blocks(turned[2 * x * length : 2 * (x + 1) * length])
        waves = product(pair(down_ref), split(points))
        for k in range(2):
            for part in range(2):
                block = waves[part * length : (part + 1) * length, k * length : (k + 1) * length]
                out_ref[:, k, part, x] = block.reshape(parts, length // parts, length)


def final_kernel(pieces_ref, x_ref, real_hbm, imag_hbm, real_ref, imag_ref, sems):
    length = real_ref.shape[-1]
    share = real_ref.shape[2]
    table = pair(x_ref)
    group = share // 2
    copies = []
    for k in range(2):
        for b in range(share):
            parts = []
            for part in range(2):
                start = (k * 2 + part) * share * share + b
                block = pieces_ref[:, pl.ds(start, share, stride=share), :]
                parts.append(block.reshape(length, length))
            turned = product(split(jnp.concatenate(parts, axis=0).T), table)
            real_ref[k, 0, b] = turned[:, :length]
            imag_ref[k, 0, b] = turned[:, length:]
            if (b + 1) % group == 0:
                done = (k, 0, pl.ds(b + 1 - group, group))
                for source, target in ((real_ref, real_hbm), (imag_ref, imag_hbm)):
                    copy = pltpu.make_async_copy(
                        source.at[done], target.at[done], sems.at[len(copies)]
                    )
                    copy.start()
                    copies.append(copy)
    for copy in copies:
        copy.wait()


def signed(positions, length):
    return jnp.where(2 * positions < length, positions, positions - length).astype(WIDE)


def line_coulomb(b, length):
    a = lax.broadcasted_iota(jnp.int32, (length, length), 0)
    c = lax.broadcasted_iota(jnp.int32, (length, length), 1)
    squared = signed(a, length) ** 2 + signed(b, length) ** 2 + signed(c, length) ** 2
    scaled = box_length**2 / math.pi / jnp.maximum(squared, 1.0)
    return jnp.where(squared > 0, scaled, 0.0) / float(length**3)


def call(body, shapes, grant=GRANT, **options):
    return pl.pallas_call(
        body,
        out_shape=jax.tree.map(
            lambda s: jax.ShapeDtypeStruct(s, WIDE),
            shapes,
            is_leaf=lambda s: isinstance(s, tuple) and isinstance(s[0], int),
        ),
        compiler_params=pltpu.CompilerParams(vmem_limit_bytes=grant),
        **options,
    )


def exchange(array, axis):
    return lax.all_to_all(array, axis, split_axis=0, concat_axis=0, tiled=True)


def partner(array, mask):
    return lax.ppermute(array, "band", [(i, i ^ mask) for i in range(lax.axis_size("band"))])


def per_device(orbitals, trials, alda_kernel, local_potential, band_energies):
    length = orbitals.shape[2]
    parts = lax.axis_size("band")
    share = length // parts
    points = share * share
    tables = {name: jnp.asarray(table) for name, table in make_tables(length).items()}
    me = lax.axis_index("band")
    place = lax.axis_index("grid")
    copies = parts // share
    kernel = line_coulomb(me * share + place // copies, length)
    own_up = lax.dynamic_slice_in_dim(tables["up"], (place % copies) * length, length, 1)

    scalar = pl.BlockSpec(memory_space=pltpu.SMEM)
    orbital_block = pl.BlockSpec((1, ROWS, length, length), lambda i: (0, i, 0, 0))
    trial_block = pl.BlockSpec((2, 1, ROWS, length, length), lambda i: (0, 0, i, 0, 0))
    table_block = pl.BlockSpec((2, 2 * length, 2 * length), lambda i: (0, 0, 0))
    share_block = pl.BlockSpec((parts, 2, ROWS, share, length), lambda i: (0, 0, i, 0, 0))
    half_block = pl.BlockSpec((parts // 2, 2, ROWS, share, length), lambda i: (0, 0, i, 0, 0))
    local_block = pl.BlockSpec((ROWS, length, length), lambda i: (i, 0, 0))
    base_block = pl.BlockSpec((2, ROWS, length, length), lambda i: (0, i, 0, 0))
    steps = (share // ROWS,)

    held = pl.BlockSpec(memory_space=pltpu.HBM)
    half = share // 2
    some = (parts // 2, 2, half, share, length)
    kept, near, pieces = call(
        density_kernel,
        [some, some, (parts, 2, half, share, length)],
        grant=WIDE_GRANT,
        in_specs=[scalar] + [held] * 4,
        out_specs=[held] * 3,
        scratch_shapes=[
            pltpu.VMEM(orbitals.shape, NARROW),
            pltpu.VMEM(trials.shape, NARROW),
            pltpu.VMEM(tables["up"].shape, NARROW),
            pltpu.VMEM(tables["down"].shape, NARROW),
            pltpu.VMEM((2, *some), WIDE),
            pltpu.VMEM((parts, 2, half, share, length), WIDE),
            pltpu.SemaphoreType.DMA((2,)),
            pltpu.SemaphoreType.DMA((2, 2)),
            pltpu.SemaphoreType.DMA((3,)),
        ],
    )(me.reshape(1), orbitals, trials, tables["up"], tables["down"])
    near = partner(near.reshape(parts // 2, points, length), 1)
    near = near + kept.reshape(parts // 2, points, length)
    near = [near[0]] + [partner(near[i], 2 * i) for i in range(1, parts // 2)]
    pieces = exchange(pieces.reshape(parts, points, length), "band")
    spectrum, lines = call(
        share_kernel, [(2 * points, length), (parts, 2 * share, length)]
    )(pieces, *near)
    lines = exchange(lines, "grid")
    held = {0: spectrum}
    for mask in (2, 4, 8):
        held[mask] = partner(spectrum, mask)
    lines = call(line_kernel, (parts, share, length))(
        lines, kernel, tables["down"], own_up
    )
    _, held[2], held[4], held[8] = lax.optimization_barrier((lines, held[2], held[4], held[8]))
    lines = exchange(lines, "grid").reshape(parts * share, length)
    both = partner(jnp.stack([held[4], held[8]]), 2)
    held[6], held[10] = both[0], both[1]
    held[12] = partner(held[8], 4)
    held[14] = partner(spectrum, 14)
    away = {}
    for masks in ((0, 2, 4, 8), (6, 10, 12, 14)):
        group = partner(jnp.stack([held[mask] for mask in masks]), 1)
        for i, mask in enumerate(masks):
            away[mask] = group[i]
    near = jnp.stack([held[mask] for mask in range(0, parts, 2)])
    far = jnp.stack([away[mask] for mask in range(0, parts, 2)])
    potential = call(spread_kernel, (parts, 2 * points, length))(lines)
    potential = exchange(potential, "band").reshape(parts, 2, share, share, length)
    base = call(
        base_kernel,
        (2, share, length, length),
        grid=steps,
        in_specs=[
            scalar, scalar, half_block, half_block, orbital_block, trial_block,
            local_block, local_block, table_block, table_block,
        ],
        out_specs=base_block,
    )(
        me.reshape(1),
        band_energies,
        near.reshape(parts // 2, 2, share, share, length),
        far.reshape(parts // 2, 2, share, share, length),
        orbitals,
        trials,
        alda_kernel,
        local_potential,
        tables["up"],
        tables["down"],
    )
    fields = call(
        field_kernel,
        (parts, 2, 2, share, share, length),
        grid=steps,
        in_specs=[share_block, orbital_block, base_block, table_block, table_block],
        out_specs=pl.BlockSpec(
            (parts, 2, 2, ROWS, share, length), lambda i: (0, 0, 0, i, 0, 0)
        ),
    )(potential, orbitals, base, tables["up"], tables["down"])
    received = exchange(fields.reshape(parts, 4 * points, length), "grid")
    shape = (2, 1, share, length, length)
    vector = pl.BlockSpec(memory_space=pltpu.VMEM)
    return tuple(
        call(
            final_kernel,
            [shape, shape],
            in_specs=[vector] * 2,
            out_specs=[pl.BlockSpec(memory_space=pltpu.HBM)] * 2,
            scratch_shapes=[
                pltpu.VMEM(shape, WIDE),
                pltpu.VMEM(shape, WIDE),
                pltpu.SemaphoreType.DMA((8,)),
            ],
        )(received, tables["last"])
    )


def solution(mesh):
    placed = (
        P("band", "grid", None, None),
        P(None, "band", "grid", None, None),
        P("grid", None, None),
        P("grid", None, None),
        P("band"),
    )

    return jax.shard_map(
        per_device,
        mesh=mesh,
        in_specs=placed,
        out_specs=(P(None, "band", "grid", None, None), P(None, "band", "grid", None, None)),
        check_vma=False,
    )
```

```python
import functools
import math

import jax
import jax.numpy as jnp
import numpy as np
from jax import lax
from jax.experimental import pallas as pl
from jax.experimental.pallas import tpu as pltpu
from jax.sharding import PartitionSpec as P


box_length = 30.0
NARROW = jnp.bfloat16
WIDE = jnp.float32
ROWS = 8
GRANT = 20 * 2**20
WIDE_GRANT = 60 * 2**20


def halves(table):
    high = table.astype(np.float32).astype(jnp.bfloat16)
    low = (table - high.astype(np.float64)).astype(np.float32).astype(jnp.bfloat16)
    return np.stack([high, low])


@functools.cache
def make_tables(length):
    wrapped = np.outer(np.arange(length), np.arange(length)) % length
    angles = wrapped.astype(np.float64) * (2.0 * math.pi / length)
    cosine, sine = np.cos(angles), np.sin(angles)
    return {
        "down": halves(np.block([[cosine, sine], [-sine, cosine]])),
        "up": halves(np.block([[cosine, -sine], [sine, cosine]])),
        "last": halves(np.block([[cosine, -sine], [sine, cosine]]) * float(length) ** -1.5),
    }


def split(value):
    high = value.astype(NARROW)
    return high, (value - high.astype(WIDE)).astype(NARROW)


def mul(left, right):
    return lax.dot_general(left, right, (((1,), (0,)), ((), ())), preferred_element_type=WIDE)


def product(left, right):
    left_high, left_low = left
    right_high, right_low = right
    return mul(left_high, right_high) + mul(left_low, right_high) + mul(left_high, right_low)


def pair(ref):
    return ref[0], ref[1]


def swap_blocks(value):
    rows, columns = value.shape[0] // 2, value.shape[1] // 2
    left = jnp.concatenate([value[:rows, :columns], value[rows:, :columns]], axis=1)
    right = jnp.concatenate([value[:rows, columns:], value[rows:, columns:]], axis=1)
    return jnp.concatenate([left, right], axis=0)


def parts_down(value):
    half = value.shape[1] // 2
    return jnp.concatenate([value[:, :half], value[:, half:]], axis=0)


def parts_across(value):
    half = value.shape[0] // 2
    return jnp.concatenate([value[:half], value[half:]], axis=1)


def density_kernel(me_ref, orbital_in, trial_in, up_in, down_in, *refs):
    (
        kept_hbm, near_hbm, out_hbm, orbital_ref, trial_ref, up_ref, down_ref, mixed_ref, out_ref,
        table_sems, row_sems, out_sems,
    ) = refs
    me = me_ref[0]
    length = orbital_ref.shape[2]
    parts, share = out_ref.shape[0], out_ref.shape[3]
    half = orbital_ref.shape[1] // 2
    tables = [
        pltpu.make_async_copy(up_in, up_ref, table_sems.at[0]),
        pltpu.make_async_copy(down_in, down_ref, table_sems.at[1]),
    ]
    rows = [pl.ds(i * half, half) for i in range(2)]
    orbitals, trials = [], []
    for i in range(2):
        part = (slice(None), rows[i])
        orbitals.append(
            pltpu.make_async_copy(orbital_in.at[part], orbital_ref.at[part], row_sems.at[i, 0])
        )
        part = (slice(None), slice(None), rows[i])
        trials.append(
            pltpu.make_async_copy(trial_in.at[part], trial_ref.at[part], row_sems.at[i, 1])
        )
    outs = [
        [
            pltpu.make_async_copy(mixed_ref.at[1], near_hbm, out_sems.at[1]),
            pltpu.make_async_copy(mixed_ref.at[0], kept_hbm, out_sems.at[0]),
        ],
        [pltpu.make_async_copy(out_ref, out_hbm, out_sems.at[2])],
    ]
    for copy in (tables[0], orbitals[0], trials[0], tables[1], orbitals[1], trials[1]):
        copy.start()
    for copy in tables:
        copy.wait()
    for i in range(2):
        orbitals[i].wait()
        trials[i].wait()
        values = []
        for x in range(half):
            orbital = 2.0 * orbital_ref[0, i * half + x].astype(WIDE)
            values.append(
                jnp.concatenate(
                    [trial_ref[k, 0, i * half + x].astype(WIDE) * orbital for k in range(2)], axis=1
                )
            )
        turned = product(split(jnp.concatenate(values, axis=0)), pair(up_ref))
        columns = [parts_down(turned[x * length : (x + 1) * length]) for x in range(half)]
        turned = product(pair(down_ref), split(jnp.concatenate(columns, axis=1)))
        for x in range(half):
            for part in range(2):
                block = turned[part * length : (part + 1) * length, x * length : (x + 1) * length]
                if i == 1:
                    out_ref[:, part, x] = block.reshape(parts, share, length)
                    continue
                for n in range(parts):
                    tile = block[n * share : (n + 1) * share]
                    mixed_ref[(n ^ me) & 1, (n ^ me) >> 1, part, x] = tile
        for copy in outs[i]:
            copy.start()
    for copy in outs[0] + outs[1]:
        copy.wait()


def share_kernel(pieces_ref, *refs):
    *near_refs, share_ref, out_ref = refs
    first = near_refs[0][...]
    for ref in near_refs[1:]:
        first = first + ref[...]
    second = pieces_ref[0]
    for i in range(1, pieces_ref.shape[0]):
        second = second + pieces_ref[i]
    rows = first.shape[0] // 2
    for part in range(2):
        held = slice(part * rows, (part + 1) * rows)
        share_ref[2 * part * rows : (2 * part + 1) * rows, :] = first[held]
        share_ref[(2 * part + 1) * rows : 2 * (part + 1) * rows, :] = second[held]
    copies, rows, _ = out_ref.shape
    share = rows // 2
    for b in range(share):
        block = share_ref[pl.ds(b, rows, stride=share), :]
        for i in range(copies // share):
            out_ref[b * (copies // share) + i] = block


def line_kernel(pieces_ref, kernel_ref, down_ref, up_ref, out_ref):
    parts, rows, length = pieces_ref.shape
    share = rows // 2
    columns = jnp.concatenate(
        [pieces_ref[:, :share, :].reshape(length, length), pieces_ref[:, share:, :].reshape(length, length)],
        axis=0,
    )
    turned = product(pair(down_ref), split(columns))
    kernel = kernel_ref[...]
    turned = turned * jnp.concatenate([kernel, kernel], axis=0)
    out_ref[...] = product(pair(up_ref), split(turned)).reshape(parts, share, length)


def spread_kernel(pieces_ref, down_ref, out_ref):
    share = pieces_ref.shape[0] // out_ref.shape[0]
    tiles = []
    for part in range(2):
        rows = [
            pieces_ref[pl.ds(part * share + x, share, stride=2 * share), :] for x in range(share)
        ]
        tiles.append(jnp.concatenate(rows, axis=0))
    value = parts_down(product(split(jnp.concatenate(tiles, axis=1)), pair(down_ref)))
    for i in range(out_ref.shape[0]):
        out_ref[i] = value


def back(blocks, up_ref, down_ref, length):
    turned = product(pair(up_ref), split(blocks))
    rows = turned.shape[1] // length
    points = [parts_across(turned[:, x * length : (x + 1) * length]) for x in range(rows)]
    return product(split(jnp.concatenate(points, axis=0)), pair(down_ref))


def base_kernel(
    me_ref, energy_ref, near_ref, far_ref, orbital_ref, trial_ref, alda_ref, local_ref,
    up_ref, down_ref, out_ref,
):
    length = orbital_ref.shape[2]
    parts = 2 * near_ref.shape[0]
    me = me_ref[0]
    energy = energy_ref[0]
    even = (me & 1) == 0
    scale = 1.0 / float(length * length)
    rows = orbital_ref.shape[1]
    columns = []
    for x in range(rows):
        tiles = []
        for part in range(2):
            for half in range(parts // 2):
                slot = half ^ (me >> 1)
                near = near_ref[slot, part, x]
                far = far_ref[slot, part, x]
                tiles.append(jnp.where(even, near, far))
                tiles.append(jnp.where(even, far, near))
        columns.append(jnp.concatenate(tiles, axis=0))
    value = back(jnp.concatenate(columns, axis=1), up_ref, down_ref, length)
    for x in range(rows):
        factor = orbital_ref[0, x].astype(WIDE) * (alda_ref[x] * scale)
        weight = local_ref[x] - energy
        for k in range(2):
            block = value[x * length : (x + 1) * length, k * length : (k + 1) * length]
            out_ref[k, x] = block * factor + weight * trial_ref[k, 0, x].astype(WIDE)


def field_kernel(potential_ref, orbital_ref, base_ref, up_ref, down_ref, out_ref):
    length = orbital_ref.shape[2]
    parts = potential_ref.shape[0]
    rows = orbital_ref.shape[1]
    columns = []
    for x in range(rows):
        columns.append(
            jnp.concatenate(
                [potential_ref[:, part, x].reshape(length, length) for part in range(2)], axis=0
            )
        )
    value = product(pair(up_ref), split(jnp.concatenate(columns, axis=1)))
    fields = []
    for x in range(rows):
        orbital = orbital_ref[0, x].astype(WIDE)
        for k in range(2):
            block = value[k * length : (k + 1) * length, x * length : (x + 1) * length]
            fields.append(block * orbital + base_ref[k, x])
    table = (up_ref[0, :length, :], up_ref[1, :length, :])
    turned = product(split(jnp.concatenate(fields, axis=0)), table)
    for x in range(rows):
        points = swap_blocks(turned[2 * x * length : 2 * (x + 1) * length])
        waves = product(pair(down_ref), split(points))
        for k in range(2):
            for part in range(2):
                block = waves[part * length : (part + 1) * length, k * length : (k + 1) * length]
                out_ref[:, k, part, x] = block.reshape(parts, length // parts, length)


def final_kernel(pieces_ref, x_ref, real_hbm, imag_hbm, real_ref, imag_ref, sems):
    length = real_ref.shape[-1]
    share = real_ref.shape[2]
    table = pair(x_ref)
    group = share // 2
    copies = []
    for k in range(2):
        for b in range(share):
            parts = []
            for part in range(2):
                start = (k * 2 + part) * share * share + b
                block = pieces_ref[:, pl.ds(start, share, stride=share), :]
                parts.append(block.reshape(length, length))
            turned = product(split(jnp.concatenate(parts, axis=0).T), table)
            real_ref[k, 0, b] = turned[:, :length]
            imag_ref[k, 0, b] = turned[:, length:]
            if (b + 1) % group == 0:
                done = (k, 0, pl.ds(b + 1 - group, group))
                for source, target in ((real_ref, real_hbm), (imag_ref, imag_hbm)):
                    copy = pltpu.make_async_copy(
                        source.at[done], target.at[done], sems.at[len(copies)]
                    )
                    copy.start()
                    copies.append(copy)
    for copy in copies:
        copy.wait()


def signed(positions, length):
    return jnp.where(2 * positions < length, positions, positions - length).astype(WIDE)


def line_coulomb(b, length):
    a = lax.broadcasted_iota(jnp.int32, (length, length), 0)
    c = lax.broadcasted_iota(jnp.int32, (length, length), 1)
    squared = signed(a, length) ** 2 + signed(b, length) ** 2 + signed(c, length) ** 2
    scaled = box_length**2 / math.pi / jnp.maximum(squared, 1.0)
    return jnp.where(squared > 0, scaled, 0.0) / float(length**3)


def call(body, shapes, grant=GRANT, **options):
    return pl.pallas_call(
        body,
        out_shape=jax.tree.map(
            lambda s: jax.ShapeDtypeStruct(s, WIDE),
            shapes,
            is_leaf=lambda s: isinstance(s, tuple) and isinstance(s[0], int),
        ),
        compiler_params=pltpu.CompilerParams(vmem_limit_bytes=grant),
        **options,
    )


def exchange(array, axis):
    return lax.all_to_all(array, axis, split_axis=0, concat_axis=0, tiled=True)


def partner(array, mask):
    return lax.ppermute(array, "band", [(i, i ^ mask) for i in range(lax.axis_size("band"))])


def per_device(orbitals, trials, alda_kernel, local_potential, band_energies):
    length = orbitals.shape[2]
    parts = lax.axis_size("band")
    share = length // parts
    points = share * share
    tables = {name: jnp.asarray(table) for name, table in make_tables(length).items()}
    me = lax.axis_index("band")
    place = lax.axis_index("grid")
    copies = parts // share
    kernel = line_coulomb(me * share + place // copies, length)
    own_up = lax.dynamic_slice_in_dim(tables["up"], (place % copies) * length, length, 1)

    scalar = pl.BlockSpec(memory_space=pltpu.SMEM)
    orbital_block = pl.BlockSpec((1, ROWS, length, length), lambda i: (0, i, 0, 0))
    trial_block = pl.BlockSpec((2, 1, ROWS, length, length), lambda i: (0, 0, i, 0, 0))
    table_block = pl.BlockSpec((2, 2 * length, 2 * length), lambda i: (0, 0, 0))
    share_block = pl.BlockSpec((parts, 2, ROWS, share, length), lambda i: (0, 0, i, 0, 0))
    half_block = pl.BlockSpec((parts // 2, 2, ROWS, share, length), lambda i: (0, 0, i, 0, 0))
    local_block = pl.BlockSpec((ROWS, length, length), lambda i: (i, 0, 0))
    base_block = pl.BlockSpec((2, ROWS, length, length), lambda i: (0, i, 0, 0))
    steps = (share // ROWS,)

    held = pl.BlockSpec(memory_space=pltpu.HBM)
    half = share // 2
    some = (parts // 2, 2, half, share, length)
    kept, near, pieces = call(
        density_kernel,
        [some, some, (parts, 2, half, share, length)],
        grant=WIDE_GRANT,
        in_specs=[scalar] + [held] * 4,
        out_specs=[held] * 3,
        scratch_shapes=[
            pltpu.VMEM(orbitals.shape, NARROW),
            pltpu.VMEM(trials.shape, NARROW),
            pltpu.VMEM(tables["up"].shape, NARROW),
            pltpu.VMEM(tables["down"].shape, NARROW),
            pltpu.VMEM((2, *some), WIDE),
            pltpu.VMEM((parts, 2, half, share, length), WIDE),
            pltpu.SemaphoreType.DMA((2,)),
            pltpu.SemaphoreType.DMA((2, 2)),
            pltpu.SemaphoreType.DMA((3,)),
        ],
    )(me.reshape(1), orbitals, trials, tables["up"], tables["down"])
    near = partner(near.reshape(parts // 2, points, length), 1)
    near = near + kept.reshape(parts // 2, points, length)
    near = [near[0]] + [partner(near[i], 2 * i) for i in range(1, parts // 2)]
    pieces = exchange(pieces.reshape(parts, points, length), "band")
    spectrum, lines = call(
        share_kernel, [(2 * points, length), (parts, 2 * share, length)]
    )(pieces, *near)
    lines = exchange(lines, "grid")
    held = {0: spectrum}
    for mask in (2, 4, 8):
        held[mask] = partner(spectrum, mask)
    lines = call(line_kernel, (parts, share, length))(
        lines, kernel, tables["down"], own_up
    )
    _, held[2], held[4], held[8] = lax.optimization_barrier((lines, held[2], held[4], held[8]))
    lines = exchange(lines, "grid").reshape(parts * share, length)
    both = partner(jnp.stack([held[4], held[8]]), 2)
    held[6], held[10] = both[0], both[1]
    held[12] = partner(held[8], 4)
    held[14] = partner(spectrum, 14)
    away = {}
    for masks in ((0, 2, 4, 8), (6, 10, 12, 14)):
        group = partner(jnp.stack([held[mask] for mask in masks]), 1)
        for i, mask in enumerate(masks):
            away[mask] = group[i]
    near = jnp.stack([held[mask] for mask in range(0, parts, 2)])
    far = jnp.stack([away[mask] for mask in range(0, parts, 2)])
    potential = call(spread_kernel, (parts, 2 * points, length))(
        lines, tables["down"]
    )
    potential = exchange(potential, "band").reshape(parts, 2, share, share, length)
    base = call(
        base_kernel,
        (2, share, length, length),
        grid=steps,
        in_specs=[
            scalar, scalar, half_block, half_block, orbital_block, trial_block,
            local_block, local_block, table_block, table_block,
        ],
        out_specs=base_block,
    )(
        me.reshape(1),
        band_energies,
        near.reshape(parts // 2, 2, share, share, length),
        far.reshape(parts // 2, 2, share, share, length),
        orbitals,
        trials,
        alda_kernel,
        local_potential,
        tables["up"],
        tables["down"],
    )
    fields = call(
        field_kernel,
        (parts, 2, 2, share, share, length),
        grid=steps,
        in_specs=[share_block, orbital_block, base_block, table_block, table_block],
        out_specs=pl.BlockSpec(
            (parts, 2, 2, ROWS, share, length), lambda i: (0, 0, 0, i, 0, 0)
        ),
    )(potential, orbitals, base, tables["up"], tables["down"])
    received = exchange(fields.reshape(parts, 4 * points, length), "grid")
    shape = (2, 1, share, length, length)
    vector = pl.BlockSpec(memory_space=pltpu.VMEM)
    return tuple(
        call(
            final_kernel,
            [shape, shape],
            in_specs=[vector] * 2,
            out_specs=[pl.BlockSpec(memory_space=pltpu.HBM)] * 2,
            scratch_shapes=[
                pltpu.VMEM(shape, WIDE),
                pltpu.VMEM(shape, WIDE),
                pltpu.SemaphoreType.DMA((8,)),
            ],
        )(received, tables["last"])
    )


def solution(mesh):
    placed = (
        P("band", "grid", None, None),
        P(None, "band", "grid", None, None),
        P("grid", None, None),
        P("grid", None, None),
        P("band"),
    )

    return jax.shard_map(
        per_device,
        mesh=mesh,
        in_specs=placed,
        out_specs=(P(None, "band", "grid", None, None), P(None, "band", "grid", None, None)),
        check_vma=False,
    )
```

```python
import functools
import math

import jax
import jax.numpy as jnp
import numpy as np
from jax import lax
from jax.experimental import pallas as pl
from jax.experimental.pallas import tpu as pltpu
from jax.sharding import PartitionSpec as P


box_length = 30.0
NARROW = jnp.bfloat16
WIDE = jnp.float32
ROWS = 8
GRANT = 20 * 2**20
WIDE_GRANT = 60 * 2**20


def halves(table):
    high = table.astype(np.float32).astype(jnp.bfloat16)
    low = (table - high.astype(np.float64)).astype(np.float32).astype(jnp.bfloat16)
    return np.stack([high, low])


@functools.cache
def make_tables(length):
    wrapped = np.outer(np.arange(length), np.arange(length)) % length
    angles = wrapped.astype(np.float64) * (2.0 * math.pi / length)
    cosine, sine = np.cos(angles), np.sin(angles)
    return {
        "down": halves(np.block([[cosine, sine], [-sine, cosine]])),
        "up": halves(np.block([[cosine, -sine], [sine, cosine]])),
        "last": halves(np.block([[cosine, -sine], [sine, cosine]]) * float(length) ** -1.5),
    }


def split(value):
    high = value.astype(NARROW)
    return high, (value - high.astype(WIDE)).astype(NARROW)


def mul(left, right):
    return lax.dot_general(left, right, (((1,), (0,)), ((), ())), preferred_element_type=WIDE)


def product(left, right):
    left_high, left_low = left
    right_high, right_low = right
    return mul(left_high, right_high) + mul(left_low, right_high) + mul(left_high, right_low)


def pair(ref):
    return ref[0], ref[1]


def swap_blocks(value):
    rows, columns = value.shape[0] // 2, value.shape[1] // 2
    left = jnp.concatenate([value[:rows, :columns], value[rows:, :columns]], axis=1)
    right = jnp.concatenate([value[:rows, columns:], value[rows:, columns:]], axis=1)
    return jnp.concatenate([left, right], axis=0)


def parts_down(value):
    half = value.shape[1] // 2
    return jnp.concatenate([value[:, :half], value[:, half:]], axis=0)


def parts_across(value):
    half = value.shape[0] // 2
    return jnp.concatenate([value[:half], value[half:]], axis=1)


def density_kernel(me_ref, orbital_in, trial_in, up_in, down_in, *refs):
    (
        kept_hbm, near_hbm, out_hbm, orbital_ref, trial_ref, up_ref, down_ref, mixed_ref, out_ref,
        table_sems, row_sems, out_sems,
    ) = refs
    me = me_ref[0]
    length = orbital_ref.shape[2]
    parts, share = out_ref.shape[0], out_ref.shape[3]
    half = orbital_ref.shape[1] // 2
    tables = [
        pltpu.make_async_copy(up_in, up_ref, table_sems.at[0]),
        pltpu.make_async_copy(down_in, down_ref, table_sems.at[1]),
    ]
    rows = [pl.ds(i * half, half) for i in range(2)]
    orbitals, trials = [], []
    for i in range(2):
        part = (slice(None), rows[i])
        orbitals.append(
            pltpu.make_async_copy(orbital_in.at[part], orbital_ref.at[part], row_sems.at[i, 0])
        )
        part = (slice(None), slice(None), rows[i])
        trials.append(
            pltpu.make_async_copy(trial_in.at[part], trial_ref.at[part], row_sems.at[i, 1])
        )
    outs = [
        [
            pltpu.make_async_copy(mixed_ref.at[1], near_hbm, out_sems.at[1]),
            pltpu.make_async_copy(mixed_ref.at[0], kept_hbm, out_sems.at[0]),
        ],
        [pltpu.make_async_copy(out_ref, out_hbm, out_sems.at[2])],
    ]
    for copy in (tables[0], orbitals[0], trials[0], tables[1], orbitals[1], trials[1]):
        copy.start()
    tables[0].wait()
    for i in range(2):
        orbitals[i].wait()
        trials[i].wait()
        values = []
        for x in range(half):
            orbital = 2.0 * orbital_ref[0, i * half + x].astype(WIDE)
            values.append(
                jnp.concatenate(
                    [trial_ref[k, 0, i * half + x].astype(WIDE) * orbital for k in range(2)], axis=1
                )
            )
        turned = product(split(jnp.concatenate(values, axis=0)), pair(up_ref))
        columns = [parts_down(turned[x * length : (x + 1) * length]) for x in range(half)]
        if i == 0:
            tables[1].wait()
        turned = product(pair(down_ref), split(jnp.concatenate(columns, axis=1)))
        for x in range(half):
            for part in range(2):
                block = turned[part * length : (part + 1) * length, x * length : (x + 1) * length]
                if i == 1:
                    out_ref[:, part, x] = block.reshape(parts, share, length)
                    continue
                for n in range(parts):
                    tile = block[n * share : (n + 1) * share]
                    mixed_ref[(n ^ me) & 1, (n ^ me) >> 1, part, x] = tile
        for copy in outs[i]:
            copy.start()
    for copy in outs[0] + outs[1]:
        copy.wait()


def share_kernel(pieces_ref, *refs):
    *near_refs, share_ref, out_ref = refs
    first = near_refs[0][...]
    for ref in near_refs[1:]:
        first = first + ref[...]
    second = pieces_ref[0]
    for i in range(1, pieces_ref.shape[0]):
        second = second + pieces_ref[i]
    rows = first.shape[0] // 2
    for part in range(2):
        held = slice(part * rows, (part + 1) * rows)
        share_ref[2 * part * rows : (2 * part + 1) * rows, :] = first[held]
        share_ref[(2 * part + 1) * rows : 2 * (part + 1) * rows, :] = second[held]
    copies, rows, _ = out_ref.shape
    share = rows // 2
    for b in range(share):
        block = share_ref[pl.ds(b, rows, stride=share), :]
        for i in range(copies // share):
            out_ref[b * (copies // share) + i] = block


def line_kernel(pieces_ref, kernel_ref, down_ref, up_ref, out_ref):
    parts, rows, length = pieces_ref.shape
    share = rows // 2
    columns = jnp.concatenate(
        [pieces_ref[:, :share, :].reshape(length, length), pieces_ref[:, share:, :].reshape(length, length)],
        axis=0,
    )
    turned = product(pair(down_ref), split(columns))
    kernel = kernel_ref[...]
    turned = turned * jnp.concatenate([kernel, kernel], axis=0)
    out_ref[...] = product(pair(up_ref), split(turned)).reshape(parts, share, length)


def spread_kernel(pieces_ref, out_ref):
    share = pieces_ref.shape[0] // out_ref.shape[0]
    for part in range(2):
        for x in range(share):
            block = pieces_ref[pl.ds(part * share + x, share, stride=2 * share), :]
            rows = pl.ds((part * share + x) * share, share)
            for i in range(out_ref.shape[0]):
                out_ref[i, rows, :] = block


def back(blocks, up_ref, down_ref, length):
    turned = product(pair(up_ref), split(blocks))
    rows = turned.shape[1] // length
    points = [parts_across(turned[:, x * length : (x + 1) * length]) for x in range(rows)]
    return product(split(jnp.concatenate(points, axis=0)), pair(down_ref))


def base_kernel(
    me_ref, energy_ref, near_ref, far_ref, orbital_ref, trial_ref, alda_ref, local_ref,
    up_ref, down_ref, out_ref,
):
    length = orbital_ref.shape[2]
    parts = 2 * near_ref.shape[0]
    me = me_ref[0]
    energy = energy_ref[0]
    even = (me & 1) == 0
    scale = 1.0 / float(length * length)
    rows = orbital_ref.shape[1]
    columns = []
    for x in range(rows):
        tiles = []
        for part in range(2):
            for half in range(parts // 2):
                slot = half ^ (me >> 1)
                near = near_ref[slot, part, x]
                far = far_ref[slot, part, x]
                tiles.append(jnp.where(even, near, far))
                tiles.append(jnp.where(even, far, near))
        columns.append(jnp.concatenate(tiles, axis=0))
    value = back(jnp.concatenate(columns, axis=1), up_ref, down_ref, length)
    for x in range(rows):
        factor = orbital_ref[0, x].astype(WIDE) * (alda_ref[x] * scale)
        weight = local_ref[x] - energy
        for k in range(2):
            block = value[x * length : (x + 1) * length, k * length : (k + 1) * length]
            out_ref[k, x] = block * factor + weight * trial_ref[k, 0, x].astype(WIDE)


def field_kernel(potential_ref, orbital_ref, base_ref, up_ref, down_ref, out_ref):
    length = orbital_ref.shape[2]
    parts = potential_ref.shape[0]
    rows = orbital_ref.shape[1]
    columns = []
    for x in range(rows):
        columns.append(
            jnp.concatenate(
                [potential_ref[:, part, x].reshape(length, length) for part in range(2)], axis=0
            )
        )
    value = back(jnp.concatenate(columns, axis=1), up_ref, down_ref, length)
    fields = []
    for x in range(rows):
        orbital = orbital_ref[0, x].astype(WIDE)
        for k in range(2):
            block = value[x * length : (x + 1) * length, k * length : (k + 1) * length]
            fields.append(block * orbital + base_ref[k, x])
    table = (up_ref[0, :length, :], up_ref[1, :length, :])
    turned = product(split(jnp.concatenate(fields, axis=0)), table)
    for x in range(rows):
        points = swap_blocks(turned[2 * x * length : 2 * (x + 1) * length])
        waves = product(pair(down_ref), split(points))
        for k in range(2):
            for part in range(2):
                block = waves[part * length : (part + 1) * length, k * length : (k + 1) * length]
                out_ref[:, k, part, x] = block.reshape(parts, length // parts, length)


def final_kernel(pieces_ref, x_ref, real_hbm, imag_hbm, real_ref, imag_ref, sems):
    length = real_ref.shape[-1]
    share = real_ref.shape[2]
    table = pair(x_ref)
    group = share // 4
    copies = []
    for k in range(2):
        for b in range(share):
            parts = []
            for part in range(2):
                start = (k * 2 + part) * share * share + b
                block = pieces_ref[:, pl.ds(start, share, stride=share), :]
                parts.append(block.reshape(length, length))
            turned = product(split(jnp.concatenate(parts, axis=0).T), table)
            real_ref[k, 0, b] = turned[:, :length]
            imag_ref[k, 0, b] = turned[:, length:]
            if (b + 1) % group == 0:
                done = (k, 0, pl.ds(b + 1 - group, group))
                for source, target in ((real_ref, real_hbm), (imag_ref, imag_hbm)):
                    copy = pltpu.make_async_copy(
                        source.at[done], target.at[done], sems.at[len(copies)]
                    )
                    copy.start()
                    copies.append(copy)
    for copy in copies:
        copy.wait()


def signed(positions, length):
    return jnp.where(2 * positions < length, positions, positions - length).astype(WIDE)


def line_coulomb(b, length):
    a = lax.broadcasted_iota(jnp.int32, (length, length), 0)
    c = lax.broadcasted_iota(jnp.int32, (length, length), 1)
    squared = signed(a, length) ** 2 + signed(b, length) ** 2 + signed(c, length) ** 2
    scaled = box_length**2 / math.pi / jnp.maximum(squared, 1.0)
    return jnp.where(squared > 0, scaled, 0.0) / float(length**3)


def call(body, shapes, grant=GRANT, **options):
    return pl.pallas_call(
        body,
        out_shape=jax.tree.map(
            lambda s: jax.ShapeDtypeStruct(s, WIDE),
            shapes,
            is_leaf=lambda s: isinstance(s, tuple) and isinstance(s[0], int),
        ),
        compiler_params=pltpu.CompilerParams(vmem_limit_bytes=grant),
        **options,
    )


def exchange(array, axis):
    return lax.all_to_all(array, axis, split_axis=0, concat_axis=0, tiled=True)


def partner(array, mask):
    return lax.ppermute(array, "band", [(i, i ^ mask) for i in range(lax.axis_size("band"))])


def per_device(orbitals, trials, alda_kernel, local_potential, band_energies):
    length = orbitals.shape[2]
    parts = lax.axis_size("band")
    share = length // parts
    points = share * share
    tables = {name: jnp.asarray(table) for name, table in make_tables(length).items()}
    me = lax.axis_index("band")
    place = lax.axis_index("grid")
    copies = parts // share
    kernel = line_coulomb(me * share + place // copies, length)
    own_up = lax.dynamic_slice_in_dim(tables["up"], (place % copies) * length, length, 1)

    scalar = pl.BlockSpec(memory_space=pltpu.SMEM)
    orbital_block = pl.BlockSpec((1, ROWS, length, length), lambda i: (0, i, 0, 0))
    trial_block = pl.BlockSpec((2, 1, ROWS, length, length), lambda i: (0, 0, i, 0, 0))
    table_block = pl.BlockSpec((2, 2 * length, 2 * length), lambda i: (0, 0, 0))
    share_block = pl.BlockSpec((parts, 2, ROWS, share, length), lambda i: (0, 0, i, 0, 0))
    half_block = pl.BlockSpec((parts // 2, 2, ROWS, share, length), lambda i: (0, 0, i, 0, 0))
    local_block = pl.BlockSpec((ROWS, length, length), lambda i: (i, 0, 0))
    base_block = pl.BlockSpec((2, ROWS, length, length), lambda i: (0, i, 0, 0))
    steps = (share // ROWS,)

    held = pl.BlockSpec(memory_space=pltpu.HBM)
    half = share // 2
    some = (parts // 2, 2, half, share, length)
    kept, near, pieces = call(
        density_kernel,
        [some, some, (parts, 2, half, share, length)],
        grant=WIDE_GRANT,
        in_specs=[scalar] + [held] * 4,
        out_specs=[held] * 3,
        scratch_shapes=[
            pltpu.VMEM(orbitals.shape, NARROW),
            pltpu.VMEM(trials.shape, NARROW),
            pltpu.VMEM(tables["up"].shape, NARROW),
            pltpu.VMEM(tables["down"].shape, NARROW),
            pltpu.VMEM((2, *some), WIDE),
            pltpu.VMEM((parts, 2, half, share, length), WIDE),
            pltpu.SemaphoreType.DMA((2,)),
            pltpu.SemaphoreType.DMA((2, 2)),
            pltpu.SemaphoreType.DMA((3,)),
        ],
    )(me.reshape(1), orbitals, trials, tables["up"], tables["down"])
    near = partner(near.reshape(parts // 2, points, length), 1)
    near = near + kept.reshape(parts // 2, points, length)
    near = [near[0]] + [partner(near[i], 2 * i) for i in range(1, parts // 2)]
    pieces = exchange(pieces.reshape(parts, points, length), "band")
    spectrum, lines = call(
        share_kernel, [(2 * points, length), (parts, 2 * share, length)]
    )(pieces, *near)
    lines = exchange(lines, "grid")
    held = {0: spectrum}
    for mask in (2, 4, 8):
        held[mask] = partner(spectrum, mask)
    lines = call(line_kernel, (parts, share, length))(
        lines, kernel, tables["down"], own_up
    )
    _, held[2], held[4], held[8] = lax.optimization_barrier((lines, held[2], held[4], held[8]))
    lines = exchange(lines, "grid").reshape(parts * share, length)
    both = partner(jnp.stack([held[4], held[8]]), 2)
    held[6], held[10] = both[0], both[1]
    held[12] = partner(held[8], 4)
    held[14] = partner(spectrum, 14)
    away = {}
    for masks in ((0, 2, 4, 8), (6, 10, 12, 14)):
        group = partner(jnp.stack([held[mask] for mask in masks]), 1)
        for i, mask in enumerate(masks):
            away[mask] = group[i]
    near = jnp.stack([held[mask] for mask in range(0, parts, 2)])
    far = jnp.stack([away[mask] for mask in range(0, parts, 2)])
    potential = call(spread_kernel, (parts, 2 * points, length))(lines)
    potential = exchange(potential, "band").reshape(parts, 2, share, share, length)
    base = call(
        base_kernel,
        (2, share, length, length),
        grid=steps,
        in_specs=[
            scalar, scalar, half_block, half_block, orbital_block, trial_block,
            local_block, local_block, table_block, table_block,
        ],
        out_specs=base_block,
    )(
        me.reshape(1),
        band_energies,
        near.reshape(parts // 2, 2, share, share, length),
        far.reshape(parts // 2, 2, share, share, length),
        orbitals,
        trials,
        alda_kernel,
        local_potential,
        tables["up"],
        tables["down"],
    )
    fields = call(
        field_kernel,
        (parts, 2, 2, share, share, length),
        grid=steps,
        in_specs=[share_block, orbital_block, base_block, table_block, table_block],
        out_specs=pl.BlockSpec(
            (parts, 2, 2, ROWS, share, length), lambda i: (0, 0, 0, i, 0, 0)
        ),
    )(potential, orbitals, base, tables["up"], tables["down"])
    received = exchange(fields.reshape(parts, 4 * points, length), "grid")
    shape = (2, 1, share, length, length)
    vector = pl.BlockSpec(memory_space=pltpu.VMEM)
    return tuple(
        call(
            final_kernel,
            [shape, shape],
            in_specs=[vector] * 2,
            out_specs=[pl.BlockSpec(memory_space=pltpu.HBM)] * 2,
            scratch_shapes=[
                pltpu.VMEM(shape, WIDE),
                pltpu.VMEM(shape, WIDE),
                pltpu.SemaphoreType.DMA((16,)),
            ],
        )(received, tables["last"])
    )


def solution(mesh):
    placed = (
        P("band", "grid", None, None),
        P(None, "band", "grid", None, None),
        P("grid", None, None),
        P("grid", None, None),
        P("band"),
    )

    return jax.shard_map(
        per_device,
        mesh=mesh,
        in_specs=placed,
        out_specs=(P(None, "band", "grid", None, None), P(None, "band", "grid", None, None)),
        check_vma=False,
    )
```
